128 devices in a mesh: part: 1, row: 16 (over z, y), col: 8 (over x, core).
Axes of the slice: x: 4, y: 4, z: 4, core: 2. Of those that a mesh axis runs over, the one named last changes fastest.
Arguments:
- ratings: float32 [2048, 65536], P(('part', 'row'), 'col')
- mask: int32 [2048, 65536], P(('part', 'row'), 'col')
- user_init: float32 [2048, 128], P(('part', 'row'))
- item_init: float32 [65536, 128], P(('part', 'col'))
Outputs:
- output 1: float32 [2048, 128], P(('part', 'row'))
- output 2: float32 [65536, 128], P(('part', 'col'))
All inputs are finite; a program needn't handle non-finite values.
Results may differ from the reference program's by a relative error of at most 0.00267786.
Values are sent between devices in bfloat16 or wider.
A program may use at most 1 GiB of HBM per device.

```python
import jax
import jax.numpy as jnp

RANK_DIM = 128
NUM_USERS = 2048
NUM_ITEMS = 65536
CG_STEPS = 4
RIDGE_WEIGHT = 0.0005


def setup_inputs(seed: int = 0, part: int = 0) -> dict:
    root_key = jax.random.fold_in(jax.random.key(seed), part)
    sub_keys = jax.random.split(root_key, 7)
    user_true = jax.random.normal(sub_keys[0], (NUM_USERS, RANK_DIM), jnp.float32)
    item_true = jax.random.normal(sub_keys[1], (NUM_ITEMS, RANK_DIM), jnp.float32)
    rating_noise = jax.random.normal(sub_keys[2], (NUM_USERS, NUM_ITEMS), jnp.float32)
    ratings = jnp.dot(user_true, item_true.T) * RANK_DIM ** -0.5 + 0.5 * rating_noise
    density = jax.random.randint(sub_keys[3], (NUM_USERS, 1), 30, 71)
    mask = (jax.random.randint(sub_keys[4], (NUM_USERS, NUM_ITEMS), 0, 100) < density).astype(jnp.int32)
    col_scale = 8.0 ** (-jnp.arange(RANK_DIM, dtype=jnp.float32) / (RANK_DIM - 1))
    item_noise = jax.random.normal(sub_keys[5], (NUM_ITEMS, RANK_DIM), jnp.float32)
    item_init = (item_true + 0.5 * item_noise) * col_scale * RANK_DIM ** -0.25
    user_init = 2.0 * jax.random.normal(sub_keys[6], (NUM_USERS, RANK_DIM), jnp.float32) * RANK_DIM ** -0.25
    return {"ratings": ratings, "mask": mask, "user_init": user_init, "item_init": item_init}


def cg_solve(mask_on, ratings, fixed_fac, start, ridge):
    fixed_bf = fixed_fac.astype(jnp.bfloat16)
    mask_bf = mask_on.astype(jnp.bfloat16)
    scores = jnp.dot(start.astype(jnp.bfloat16), fixed_bf.T, preferred_element_type=jnp.float32)
    resid_obs = jnp.where(mask_on, ratings - scores, 0.0).astype(jnp.bfloat16)
    residual = jnp.dot(resid_obs, fixed_bf, preferred_element_type=jnp.float32) - ridge * start
    direction = residual
    estimate = start
    res_sq = jnp.sum(residual * residual, axis=1, keepdims=True)
    for cg_step in range(CG_STEPS):
        scores = jnp.dot(direction.astype(jnp.bfloat16), fixed_bf.T, preferred_element_type=jnp.float32)
        masked = mask_bf * scores.astype(jnp.bfloat16)
        gram_dir = jnp.dot(masked, fixed_bf, preferred_element_type=jnp.float32) + ridge * direction
        step_size = res_sq / jnp.sum(direction * gram_dir, axis=1, keepdims=True)
        estimate = estimate + step_size * direction
        if cg_step + 1 < CG_STEPS:
            residual = residual - step_size * gram_dir
            new_sq = jnp.sum(residual * residual, axis=1, keepdims=True)
            direction = residual + (new_sq / res_sq) * direction
            res_sq = new_sq
    return estimate


def reference(ratings, mask, user_init, item_init):
    mask_on = mask > 0
    user_new = cg_solve(mask_on, ratings, item_init, user_init, RIDGE_WEIGHT * NUM_ITEMS)
    item_new = cg_solve(mask_on.T, ratings.T, user_new, item_init, RIDGE_WEIGHT * NUM_USERS)
    return (user_new, item_new)
```

```python
import jax
import jax.numpy as jnp
from jax import lax
from jax.experimental import pallas as pl
from jax.experimental.pallas import tpu as pltpu
from jax.sharding import PartitionSpec as P

CG_STEPS = 4
RIDGE_WEIGHT = 0.0005
MESH = pl.DeviceIdType.MESH
F32 = jnp.float32
BF16 = jnp.bfloat16

NZ = NY = 4
NROW = NZ * NY
NCOL = 8
CHUNKS = 2
OFFSETS = sorted(
    [(dz, dy) for dz in range(NZ) for dy in range(NY) if dz or dy],
    key=lambda o: min(o[0], NZ - o[0]) + min(o[1], NY - o[1]),
)


def dot(a, b, ca, cb):
    return lax.dot_general(a, b, (((ca,), (cb,)), ((), ())), preferred_element_type=F32)


def kernel(
    ratings, mask, user_init, item_init, user_out, item_out,
    r_in, m_in, v_in, w_in, fixed, mask_bf, r_send, r_recv, mask_items,
    part_sums, rs_recv, p_all, w_all, fw, fw_t, v_all,
    in_sem, w_in_sem, v_in_sem, a2a_send, a2a_recv, rs_send_sem, rs_recv_sem, ag_send, ag_recv,
    wc_send, wc_recv, wr_send, wr_recv, vg_send, vg_recv, out_sem, wout_sem,
):
    users, items = r_in.shape
    rank = w_in.shape[1]
    own_users = users // NCOL
    own_items = items // NROW
    all_users = users * NROW
    row = lax.axis_index("row")
    col = lax.axis_index("col")
    zi = row // NY
    yi = lax.rem(row, NY)
    ridge_user = RIDGE_WEIGHT * items * NCOL
    ridge_item = RIDGE_WEIGHT * all_users

    def row_of(dz, dy):
        return lax.rem(zi + dz, NZ) * NY + lax.rem(yi + dy, NY)

    def row_dev(r):
        return (0, r, col)

    def col_dev(k):
        return (0, row, lax.rem(col + k, NCOL))

    def remote(src, dst, send, recv, dev):
        return pltpu.make_async_remote_copy(
            src_ref=src, dst_ref=dst, send_sem=send, recv_sem=recv, device_id=dev, device_id_type=MESH
        )

    barrier = pltpu.get_barrier_semaphore()
    for dz, dy in OFFSETS:
        pl.semaphore_signal(barrier, inc=1, device_id=row_dev(row_of(dz, dy)), device_id_type=MESH)
    for k in range(1, NCOL):
        pl.semaphore_signal(barrier, inc=1, device_id=col_dev(k), device_id_type=MESH)

    order = OFFSETS + [(0, 0)]
    loads = []
    for k, (dz, dy) in enumerate(order):
        cols = pl.ds(pl.multiple_of(row_of(dz, dy) * own_items, own_items), own_items)
        a = pltpu.make_async_copy(ratings.at[:, cols], r_in.at[:, cols], in_sem.at[0, k])
        b = pltpu.make_async_copy(mask.at[:, cols], m_in.at[:, cols], in_sem.at[1, k])
        a.start()
        b.start()
        loads.append((a, b, cols))
    w_load = pltpu.make_async_copy(user_init, w_in, w_in_sem)
    w_load.start()
    v_load = pltpu.make_async_copy(item_init, v_in, v_in_sem)
    v_load.start()

    pl.semaphore_wait(barrier, len(OFFSETS) + NCOL - 1)

    my_users = pl.ds(pl.multiple_of(row * users, users), users)
    exchange = []
    for k, (dz, dy) in enumerate(order):
        a, b, cols = loads[k]
        a.wait()
        b.wait()
        on = m_in[:, cols] > 0
        mask_bf[:, cols] = on.astype(F32).astype(BF16)
        marked = jnp.where(on, r_in[:, cols], jnp.inf)
        if (dz, dy) == (0, 0):
            r_recv[my_users, :] = marked
        else:
            r_send[k] = marked
            c = remote(r_send.at[k], r_recv.at[my_users, :], a2a_send.at[k], a2a_recv.at[k], row_dev(row_of(dz, dy)))
            c.start()
            exchange.append(c)

    w_load.wait()
    v_load.wait()
    tile = items // 8
    fixed[...] = v_in[...].astype(BF16)

    def reduce_users(it, acc):
        part_sums[it] = acc
        copies = []
        for k in range(1, NCOL):
            peer = lax.rem(col + k, NCOL)
            c = remote(
                part_sums.at[it, pl.ds(pl.multiple_of(peer * own_users, own_users), own_users)],
                rs_recv.at[it, k - 1], rs_send_sem.at[it, k - 1], rs_recv_sem.at[it, k - 1], col_dev(k),
            )
            c.start()
            copies.append(c)
        total = part_sums[it, mine, :]
        for k in range(1, NCOL):
            copies[k - 1].wait()
            total = total + rs_recv[it, k - 1]
        return total

    def share_direction(it, p):
        p_all[it, mine, :] = p.astype(BF16)
        copies = []
        for k in range(1, NCOL):
            c = remote(
                p_all.at[it, mine], p_all.at[it, mine], ag_send.at[it, k - 1], ag_recv.at[it, k - 1], col_dev(k)
            )
            c.start()
            copies.append(c)
        for c in copies:
            c.wait()

    def user_product(it):
        p = p_all[it]
        acc = jnp.zeros((users, rank), F32)
        for t in range(8):
            f = fixed[t * tile:(t + 1) * tile, :]
            z = dot(p, f, 1, 1).astype(BF16) * mask_bf[:, t * tile:(t + 1) * tile]
            acc = acc + dot(z, f, 1, 0)
        return acc

    mine = pl.ds(pl.multiple_of(col * own_users, own_users), own_users)
    w_bf = w_in[...].astype(BF16)
    acc = jnp.zeros((users, rank), F32)
    for t in range(8):
        cols = slice(t * tile, (t + 1) * tile)
        f = fixed[cols, :]
        d = jnp.where(m_in[:, cols] > 0, r_in[:, cols] - dot(w_bf, f, 1, 1), 0.0).astype(BF16)
        acc = acc + dot(d, f, 1, 0)
    x = w_in[mine, :]
    r = reduce_users(0, acc) - ridge_user * x
    p = r
    rr = jnp.sum(r * r, axis=1, keepdims=True)
    share_direction(0, p)

    def user_step(it, state):
        x, r, p, rr = state
        q = reduce_users(it, user_product(it - 1)) + ridge_user * p
        a = rr / jnp.sum(p * q, axis=1, keepdims=True)
        x = x + a * p
        r = r - a * q
        rn = jnp.sum(r * r, axis=1, keepdims=True)
        p = r + (rn / rr) * p
        share_direction(it, p)
        return x, r, p, rn

    x, r, p, rr = lax.fori_loop(1, CG_STEPS, user_step, (x, r, p, rr))
    q = reduce_users(CG_STEPS, user_product(CG_STEPS - 1)) + ridge_user * p
    a = rr / jnp.sum(p * q, axis=1, keepdims=True)
    x = x + a * p

    w_all[mine, :] = x
    copies = []
    for k in range(1, NCOL):
        c = remote(w_all.at[mine], w_all.at[mine], wc_send.at[k - 1], wc_recv.at[k - 1], col_dev(k))
        c.start()
        copies.append(c)
    for c in copies:
        c.wait()
    w_out = pltpu.make_async_copy(w_all, user_out, wout_sem)
    w_out.start()
    fw[my_users, :] = w_all[...].astype(BF16)
    shared = []
    for k, (dz, dy) in enumerate(OFFSETS):
        c = remote(fw.at[my_users], fw.at[my_users], wr_send.at[k], wr_recv.at[k], row_dev(row_of(dz, dy)))
        c.start()
        shared.append(c)

    for c in exchange:
        c.wait()
    step = all_users // 8
    for t in range(8):
        rows = slice(t * step, (t + 1) * step)
        mask_items[rows, :] = jnp.where(r_recv[rows, :] < jnp.inf, 1.0, 0.0).astype(BF16)
    x_all = v_in[pl.ds(pl.multiple_of(row * own_items, own_items), own_items), :].T
    for c in shared:
        c.wait()
    fw_t[...] = fw[...].astype(F32).T.astype(BF16)

    width = own_items // CHUNKS
    half = width // 2
    tall = all_users // 4

    def item_product(p_bf, cols, first):
        acc = jnp.zeros((rank, width), F32)
        for t in range(4):
            rows = slice(t * tall, (t + 1) * tall)
            s = dot(fw[rows, :], p_bf, 1, 0)
            if first:
                known = r_recv[rows, cols]
                z = jnp.where(known < jnp.inf, known - s, 0.0).astype(BF16)
            else:
                z = s.astype(BF16) * mask_items[rows, cols]
            acc = acc + dot(fw_t[:, rows], z, 1, 0)
        return acc

    def block(r, q, h):
        return pl.ds(pl.multiple_of(r * own_items + q * width + h * half, half), half)

    def halfblock(r, q, h, part):
        n = half // 2
        return pl.ds(pl.multiple_of(r * own_items + q * width + h * half + part * n, n), n)

    dims = [((0, 1), (1, 0)), ((1, 0), (0, 1))]

    def scaled(d, n):
        return (d[0] * n % NZ, d[1] * n % NY)

    def added(d, e):
        return ((d[0] + e[0]) % NZ, (d[1] + e[1]) % NY)

    started = []

    def send(rows, dev, q, h, slot):
        c = remote(v_all.at[rows], v_all.at[rows], vg_send.at[q, h, slot], vg_recv.at[q, h, slot], dev)
        c.start()
        started.append(c)
        return c

    def gather_own(q):
        got = {}
        for h in range(2):
            d1, d2 = dims[h]
            for s, sign in enumerate((1, 3)):
                got[h, 0, s] = send(block(row, q, h), row_dev(row_of(*scaled(d1, sign))), q, h, s)
            for s, sign in enumerate((1, 3)):
                got[h, 1, 0, s] = send(block(row, q, h), row_dev(row_of(*scaled(d2, sign))), q, h, 4 + s)
        return got

    def gather_first(q, got):
        for s, sign in enumerate((1, 3)):
            for h in range(2):
                d1, d2 = dims[h]
                got[h, 0, s].wait_recv()
                src = row_of(*scaled(d1, 4 - sign))
                got[h, 2, s] = send(
                    halfblock(src, q, h, s), row_dev(row_of(*scaled(d1, sign))), q, h, 2 + s
                )
                for s2, sign2 in enumerate((1, 3)):
                    got[h, 1, 1 + s, s2] = send(
                        block(src, q, h), row_dev(row_of(*scaled(d2, sign2))), q, h, 6 + 2 * s + s2
                    )
        for h in range(2):
            d1, d2 = dims[h]
            got[h, 2, 0].wait_recv()
            got[h, 2, 1].wait_recv()
            src = row_of(*scaled(d1, 2))
            for s2, sign2 in enumerate((1, 3)):
                got[h, 1, 3, s2] = send(block(src, q, h), row_dev(row_of(*scaled(d2, sign2))), q, h, 10 + s2)

    def gather_second(q, got, b):
        for h in range(2):
            d1, d2 = dims[h]
            base = scaled(d1, (0, 3, 1, 2)[b])
            for s, sign in enumerate((1, 3)):
                got[h, 1, b, s].wait_recv()
                src = row_of(*added(base, scaled(d2, 4 - sign)))
                got[h, 3, b, s] = send(
                    halfblock(src, q, h, s), row_dev(row_of(*scaled(d2, sign))), q, h, 12 + 2 * b + s
                )

    pending = []
    for q in range(CHUNKS):
        cols = slice(q * width, (q + 1) * width)
        x = x_all[:, cols]
        r = item_product(x.astype(BF16), cols, True) - ridge_item * x
        p = r
        rr = jnp.sum(r * r, axis=0, keepdims=True)

        def item_step(_, state):
            x, r, p, rr = state
            q = item_product(p.astype(BF16), cols, False) + ridge_item * p
            a = rr / jnp.sum(p * q, axis=0, keepdims=True)
            x = x + a * p
            r = r - a * q
            rn = jnp.sum(r * r, axis=0, keepdims=True)
            p = r + (rn / rr) * p
            return x, r, p, rn

        x, r, p, rr = lax.fori_loop(0, CG_STEPS - 1, item_step, (x, r, p, rr))
        qv = item_product(p.astype(BF16), cols, False) + ridge_item * p
        x = x + rr / jnp.sum(p * qv, axis=0, keepdims=True) * p
        v_all[pl.ds(pl.multiple_of(row * own_items + q * width, width), width), :] = x.T
        pending.append(gather_own(q))

    for q in range(CHUNKS):
        gather_first(q, pending[q])
    for b in range(4):
        for q in range(CHUNKS):
            gather_second(q, pending[q], b)
    for q in range(CHUNKS):
        for h in range(2):
            for b in range(4):
                for s in range(2):
                    pending[q][h, 3, b, s].wait_recv()
    for c in started:
        c.wait_send()
    v_out = pltpu.make_async_copy(v_all, item_out, out_sem)
    v_out.start()
    v_out.wait()
    w_out.wait()


def solution(mesh):
    grid_spec = P(("part", "row"), "col")
    user_spec = P(("part", "row"), None)
    item_spec = P(("part", "col"), None)

    def local_step(ratings, mask, user_init, item_init):
        users, items = ratings.shape
        rank = user_init.shape[1]
        own_users = users // NCOL
        own_items = items // NROW
        all_users = users * NROW
        peers = len(OFFSETS)
        dma = pltpu.SemaphoreType.DMA
        hbm = pl.BlockSpec(memory_space=pl.ANY)
        return pl.pallas_call(
            kernel,
            out_shape=(
                jax.ShapeDtypeStruct((users, rank), F32),
                jax.ShapeDtypeStruct((items, rank), F32),
            ),
            in_specs=[hbm] * 4,
            out_specs=(hbm, hbm),
            scratch_shapes=[
                pltpu.VMEM((users, items), F32),
                pltpu.VMEM((users, items), jnp.int32),
                pltpu.VMEM((items, rank), F32),
                pltpu.VMEM((users, rank), F32),
                pltpu.VMEM((items, rank), BF16),
                pltpu.VMEM((users, items), BF16),
                pltpu.VMEM((peers, users, own_items), F32),
                pltpu.VMEM((all_users, own_items), F32),
                pltpu.VMEM((all_users, own_items), BF16),
                pltpu.VMEM((CG_STEPS + 1, users, rank), F32),
                pltpu.VMEM((CG_STEPS + 1, NCOL - 1, own_users, rank), F32),
                pltpu.VMEM((CG_STEPS, users, rank), BF16),
                pltpu.VMEM((users, rank), F32),
                pltpu.VMEM((all_users, rank), BF16),
                pltpu.VMEM((rank, all_users), BF16),
                pltpu.VMEM((items, rank), F32),
                dma((2, NROW)),
                dma,
                dma,
                dma((peers,)),
                dma((peers,)),
                dma((CG_STEPS + 1, NCOL - 1)),
                dma((CG_STEPS + 1, NCOL - 1)),
                dma((CG_STEPS, NCOL - 1)),
                dma((CG_STEPS, NCOL - 1)),
                dma((NCOL - 1,)),
                dma((NCOL - 1,)),
                dma((peers,)),
                dma((peers,)),
                dma((CHUNKS, 2, 20)),
                dma((CHUNKS, 2, 20)),
                dma,
                dma,
            ],
            compiler_params=pltpu.CompilerParams(
                collective_id=0, has_side_effects=True, vmem_limit_bytes=60 * 2**20
            ),
            name="als_sweep",
        )(ratings, mask, user_init, item_init)

    return jax.shard_map(
        local_step,
        mesh=mesh,
        in_specs=(grid_spec, grid_spec, user_spec, item_spec),
        out_specs=(user_spec, item_spec),
        check_vma=False,
    )
```

```python
import jax
import jax.numpy as jnp
from jax import lax
from jax.experimental import pallas as pl
from jax.experimental.pallas import tpu as pltpu
from jax.sharding import PartitionSpec as P

CG_STEPS = 4
RIDGE_WEIGHT = 0.0005
MESH = pl.DeviceIdType.MESH
F32 = jnp.float32
BF16 = jnp.bfloat16

NZ = NY = 4
NROW = NZ * NY
NX = 4
NCOL = NX * 2
CHUNKS = 2
OFFSETS = [
    (1, 1), (3, 3), (1, 0), (3, 0), (2, 1), (2, 3), (2, 0), (1, 3), (3, 1), (1, 2), (3, 2), (2, 2), (0, 1), (0, 3), (0, 2),
]
NEAR_FIRST = sorted(
    range(len(OFFSETS)), key=lambda k: min(OFFSETS[k][0], NZ - OFFSETS[k][0]) + min(OFFSETS[k][1], NY - OFFSETS[k][1])
)


def dot(a, b, ca, cb):
    return lax.dot_general(a, b, (((ca,), (cb,)), ((), ())), preferred_element_type=F32)


def kernel(
    ratings, mask, user_init, item_init, user_out, item_out,
    r_in, m_in, v_in, w_in, fixed, fixed_t, mask_bf, r_send, r_recv, mask_items,
    pair_send, pair_recv, chip_sum, x_recv, p_all, fw, fw_t,
    in_sem, w_in_sem, v_in_sem, a2a_send, a2a_recv, pair_send_sem, pair_recv_sem, x_send_sem, x_recv_sem,
    ag_send, ag_recv, wc_send, wc_recv, wr_send, wr_recv, wf_send, wf_recv, vg_send, vg_recv,
):
    users, items = r_in.shape
    rank = w_in.shape[1]
    half_users = users // 2
    own_items = items // NROW
    all_users = users * NROW
    width = own_items // CHUNKS
    half = width // 2
    tall = all_users // 4
    tile = items // 8
    row = lax.axis_index("row")
    col = lax.axis_index("col")
    zi = row // NY
    yi = lax.rem(row, NY)
    xi = col // 2
    core = lax.rem(col, 2)
    ridge_user = RIDGE_WEIGHT * items * NCOL
    ridge_item = RIDGE_WEIGHT * all_users
    partner = (0, row, xi * 2 + 1 - core)

    def row_of(dz, dy):
        return lax.rem(zi + dz, NZ) * NY + lax.rem(yi + dy, NY)

    def row_dev(r):
        return (0, r, col)

    def x_dev(k):
        return (0, row, lax.rem(xi + k, NX) * 2 + core)

    def remote(src, dst, send, recv, dev):
        return pltpu.make_async_remote_copy(
            src_ref=src, dst_ref=dst, send_sem=send, recv_sem=recv, device_id=dev, device_id_type=MESH
        )

    peers = [row_dev(row_of(dz, dy)) for dz, dy in OFFSETS] + [x_dev(k) for k in range(1, NX)] + [partner]
    barrier = pltpu.get_barrier_semaphore()
    for dev in peers:
        pl.semaphore_signal(barrier, inc=1, device_id=dev, device_id_type=MESH)

    order = OFFSETS + [(0, 0)]
    loads = []
    for k, (dz, dy) in enumerate(order):
        cols = pl.ds(pl.multiple_of(row_of(dz, dy) * own_items, own_items), own_items)
        a = pltpu.make_async_copy(ratings.at[:, cols], r_in.at[:, cols], in_sem.at[0, k])
        b = pltpu.make_async_copy(mask.at[:, cols], m_in.at[:, cols], in_sem.at[1, k])
        a.start()
        b.start()
        loads.append((a, b, cols))
    w_load = pltpu.make_async_copy(user_init, w_in, w_in_sem)
    w_load.start()
    v_loads = []
    for t in range(8):
        c = pltpu.make_async_copy(
            item_init.at[t * tile:(t + 1) * tile], v_in.at[t * tile:(t + 1) * tile], v_in_sem.at[t]
        )
        c.start()
        v_loads.append(c)

    my_users = pl.ds(pl.multiple_of(row * users, users), users)
    exchange = {}

    def exchange_start(k, q):
        dz, dy = order[k]
        c = remote(
            r_send.at[q, k], r_recv.at[q, my_users, :], a2a_send.at[q, k], a2a_recv.at[q, k],
            row_dev(row_of(dz, dy)),
        )
        c.start()
        exchange[q, k] = c

    ahead = 4
    for k, (dz, dy) in enumerate(order):
        a, b, cols = loads[k]
        a.wait()
        b.wait()
        on = m_in[:, cols] > 0
        mask_bf[:, cols] = on.astype(F32).astype(BF16)
        marked = jnp.where(on, r_in[:, cols], jnp.inf)
        for q in range(CHUNKS):
            if (dz, dy) == (0, 0):
                r_recv[q, my_users, :] = marked[:, q * width:(q + 1) * width]
            else:
                r_send[q, k] = marked[:, q * width:(q + 1) * width]
        if k == ahead - 1:
            pl.semaphore_wait(barrier, len(peers))
            for j in range(ahead):
                exchange_start(j, 0)
        elif k >= ahead and k < len(OFFSETS):
            exchange_start(k, 0)
    for q in range(1, CHUNKS):
        for k in range(len(OFFSETS)):
            exchange_start(k, q)

    mine = pl.ds(pl.multiple_of(core * half_users, half_users), half_users)
    other = pl.ds(pl.multiple_of((1 - core) * half_users, half_users), half_users)

    def reduce_users(it, product, meanwhile=None):
        pair_send[it] = product(other)
        c = remote(pair_send.at[it], pair_recv.at[it], pair_send_sem.at[it], pair_recv_sem.at[it], partner)
        c.start()
        own = product(mine)
        c.wait()
        own = own + pair_recv[it]
        chip_sum[it] = own
        copies = []
        for k in (2, 1, 3):
            c = remote(
                chip_sum.at[it], x_recv.at[it, k - 1], x_send_sem.at[it, k - 1], x_recv_sem.at[it, k - 1], x_dev(k)
            )
            c.start()
            copies.append(c)
        if meanwhile is not None:
            meanwhile()
        for c in copies:
            c.wait()
        return (own + x_recv[it, 1]) + (x_recv[it, 0] + x_recv[it, 2])

    def share_direction(it, p):
        p_all[it, mine, :] = p.astype(BF16)
        c = remote(p_all.at[it, mine], p_all.at[it, mine], ag_send.at[it], ag_recv.at[it], partner)
        c.start()
        c.wait()

    def user_product(it):
        def product(rows):
            p = p_all[it, rows, :]
            acc = jnp.zeros((half_users, rank), F32)
            for t in range(8):
                cols = slice(t * tile, (t + 1) * tile)
                z = dot(p, fixed_t[:, cols], 1, 0).astype(BF16) * mask_bf[rows, cols]
                acc = acc + dot(z, fixed[cols, :], 1, 0)
            return acc
        return product

    w_load.wait()
    ready = []

    def user_residual(rows):
        w = w_in[rows, :].astype(BF16)
        acc = jnp.zeros((half_users, rank), F32)
        for t in range(8):
            cols = slice(t * tile, (t + 1) * tile)
            if len(ready) <= t:
                v_loads[t].wait()
                fixed[cols, :] = v_in[cols, :].astype(BF16)
                ready.append(t)
            f = fixed[cols, :]
            d = jnp.where(m_in[rows, cols] > 0, r_in[rows, cols] - dot(w, f, 1, 1), 0.0).astype(BF16)
            acc = acc + dot(d, f, 1, 0)
        return acc

    def transpose_fixed():
        for t in range(8):
            cols = slice(t * tile, (t + 1) * tile)
            fixed_t[:, cols] = fixed[cols, :].T

    x = w_in[mine, :]
    r = reduce_users(0, user_residual, transpose_fixed) - ridge_user * x
    p = r
    rr = jnp.sum(r * r, axis=1, keepdims=True)
    share_direction(0, p)

    def user_step(it, state):
        x, r, p, rr = state
        q = reduce_users(it, user_product(it - 1)) + ridge_user * p
        a = rr / jnp.sum(p * q, axis=1, keepdims=True)
        x = x + a * p
        r = r - a * q
        rn = jnp.sum(r * r, axis=1, keepdims=True)
        p = r + (rn / rr) * p
        share_direction(it, p)
        return x, r, p, rn

    x, r, p, rr = lax.fori_loop(1, CG_STEPS, user_step, (x, r, p, rr))
    q = reduce_users(CG_STEPS, user_product(CG_STEPS - 1)) + ridge_user * p
    a = rr / jnp.sum(p * q, axis=1, keepdims=True)
    x = x + a * p

    def user_block(r):
        return pl.ds(pl.multiple_of(r * users + core * half_users, half_users), half_users)

    fw[user_block(row), :] = x.astype(BF16)
    shared = {}
    for k in reversed(NEAR_FIRST):
        blk = user_block(row)
        c = remote(fw.at[blk], fw.at[blk], wr_send.at[k], wr_recv.at[k], row_dev(row_of(*OFFSETS[k])))
        c.start()
        shared[k] = c
    crossed = [remote(fw.at[user_block(row)], fw.at[user_block(row)], wf_send.at[NROW - 1], wf_recv.at[NROW - 1], partner)]
    crossed[0].start()
    user_out[mine, :] = x
    w_copy = remote(user_out.at[mine], user_out.at[mine], wc_send, wc_recv, partner)
    w_copy.start()

    def item_mask(q):
        for k in range(len(OFFSETS)):
            exchange[q, k].wait()
        for t in range(4):
            rows = slice(t * tall, (t + 1) * tall)
            mask_items[q, rows, :] = jnp.where(r_recv[q, rows, :] < jnp.inf, 1.0, 0.0).astype(BF16)

    x_all = v_in[pl.ds(pl.multiple_of(row * own_items, own_items), own_items), :].T
    item_mask(0)
    sources = [row]
    for k in NEAR_FIRST:
        shared[k].wait()
        src = row_of(NZ - OFFSETS[k][0], NY - OFFSETS[k][1])
        c = remote(fw.at[user_block(src)], fw.at[user_block(src)], wf_send.at[k], wf_recv.at[k], partner)
        c.start()
        crossed.append(c)
        sources.append(src)
    for c, src in zip(crossed, sources):
        c.wait()
        blk = pl.ds(pl.multiple_of(src * users, users), users)
        fw_t[:, blk] = fw[blk, :].T

    def item_product(p_bf, q, first):
        acc = jnp.zeros((rank, width), F32)
        for t in range(4):
            rows = slice(t * tall, (t + 1) * tall)
            s = dot(fw[rows, :], p_bf, 1, 0)
            if first:
                known = r_recv[q, rows, :]
                z = jnp.where(known < jnp.inf, known - s, 0.0).astype(BF16)
            else:
                z = s.astype(BF16) * mask_items[q, rows, :]
            acc = acc + dot(fw_t[:, rows], z, 1, 0)
        return acc

    def block(r, q, h):
        return pl.ds(pl.multiple_of(r * own_items + q * width + h * half, half), half)

    def halfblock(r, q, h, part):
        n = half // 2
        return pl.ds(pl.multiple_of(r * own_items + q * width + h * half + part * n, n), n)

    dims = [((0, 1), (1, 0)), ((1, 0), (0, 1))]

    def scaled(d, n):
        return (d[0] * n % NZ, d[1] * n % NY)

    def added(d, e):
        return ((d[0] + e[0]) % NZ, (d[1] + e[1]) % NY)

    started = []

    def send(rows, dev, q, h, slot):
        c = remote(item_out.at[rows], item_out.at[rows], vg_send.at[q, h, slot], vg_recv.at[q, h, slot], dev)
        c.start()
        started.append(c)
        return c

    def gather_own(q):
        got = {}
        for h in range(2):
            d1, d2 = dims[h]
            for s, sign in enumerate((1, 3)):
                got[h, 0, s] = send(block(row, q, h), row_dev(row_of(*scaled(d1, sign))), q, h, s)
            for s, sign in enumerate((1, 3)):
                got[h, 1, 0, s] = send(block(row, q, h), row_dev(row_of(*scaled(d2, sign))), q, h, 4 + s)
        return got

    def gather_first(q, got):
        for s, sign in enumerate((1, 3)):
            for h in range(2):
                d1, d2 = dims[h]
                got[h, 0, s].wait_recv()
                src = row_of(*scaled(d1, 4 - sign))
                got[h, 2, s] = send(
                    halfblock(src, q, h, s), row_dev(row_of(*scaled(d1, sign))), q, h, 2 + s
                )
                for s2, sign2 in enumerate((1, 3)):
                    got[h, 1, 1 + s, s2] = send(
                        block(src, q, h), row_dev(row_of(*scaled(d2, sign2))), q, h, 6 + 2 * s + s2
                    )
        for h in range(2):
            d1, d2 = dims[h]
            got[h, 2, 0].wait_recv()
            got[h, 2, 1].wait_recv()
            src = row_of(*scaled(d1, 2))
            for s2, sign2 in enumerate((1, 3)):
                got[h, 1, 3, s2] = send(block(src, q, h), row_dev(row_of(*scaled(d2, sign2))), q, h, 10 + s2)

    def gather_second(q, got, b):
        for h in range(2):
            d1, d2 = dims[h]
            base = scaled(d1, (0, 3, 1, 2)[b])
            for s, sign in enumerate((1, 3)):
                got[h, 1, b, s].wait_recv()
                src = row_of(*added(base, scaled(d2, 4 - sign)))
                got[h, 3, b, s] = send(
                    halfblock(src, q, h, s), row_dev(row_of(*scaled(d2, sign))), q, h, 12 + 2 * b + s
                )

    pending = []
    for q in range(CHUNKS):
        if q:
            item_mask(q)
        x = x_all[:, q * width:(q + 1) * width]
        r = item_product(x.astype(BF16), q, True) - ridge_item * x
        p = r
        rr = jnp.sum(r * r, axis=0, keepdims=True)

        def item_step(_, state):
            x, r, p, rr = state
            g = item_product(p.astype(BF16), q, False) + ridge_item * p
            a = rr / jnp.sum(p * g, axis=0, keepdims=True)
            x = x + a * p
            r = r - a * g
            rn = jnp.sum(r * r, axis=0, keepdims=True)
            p = r + (rn / rr) * p
            return x, r, p, rn

        x, r, p, rr = lax.fori_loop(0, CG_STEPS - 1, item_step, (x, r, p, rr))
        g = item_product(p.astype(BF16), q, False) + ridge_item * p
        x = x + (rr / jnp.sum(p * g, axis=0, keepdims=True)) * p
        item_out[pl.ds(pl.multiple_of(row * own_items + q * width, width), width), :] = x.T
        pending.append(gather_own(q))

    for q in range(CHUNKS):
        gather_first(q, pending[q])
    for b in range(4):
        for q in range(CHUNKS):
            gather_second(q, pending[q], b)
    for q in range(CHUNKS):
        for h in range(2):
            for b in range(4):
                for s in range(2):
                    pending[q][h, 3, b, s].wait_recv()
    for c in started:
        c.wait_send()
    w_copy.wait()


def solution(mesh):
    grid_spec = P(("part", "row"), "col")
    user_spec = P(("part", "row"), None)
    item_spec = P(("part", "col"), None)

    def local_step(ratings, mask, user_init, item_init):
        users, items = ratings.shape
        rank = user_init.shape[1]
        own_items = items // NROW
        all_users = users * NROW
        width = own_items // CHUNKS
        half_users = users // 2
        peers = len(OFFSETS)
        dma = pltpu.SemaphoreType.DMA
        hbm = pl.BlockSpec(memory_space=pltpu.HBM)
        vmem = pl.BlockSpec(memory_space=pltpu.VMEM)
        return pl.pallas_call(
            kernel,
            out_shape=(pltpu.VMEM((users, rank), F32), pltpu.VMEM((items, rank), F32)),
            in_specs=[hbm] * 4,
            out_specs=(vmem, vmem),
            scratch_shapes=[
                pltpu.VMEM((users, items), F32),
                pltpu.VMEM((users, items), jnp.int32),
                pltpu.VMEM((items, rank), F32),
                pltpu.VMEM((users, rank), F32),
                pltpu.VMEM((items, rank), BF16),
                pltpu.VMEM((rank, items), BF16),
                pltpu.VMEM((users, items), BF16),
                pltpu.VMEM((CHUNKS, peers, users, width), F32),
                pltpu.VMEM((CHUNKS, all_users, width), F32),
                pltpu.VMEM((CHUNKS, all_users, width), BF16),
                pltpu.VMEM((CG_STEPS + 1, half_users, rank), F32),
                pltpu.VMEM((CG_STEPS + 1, half_users, rank), F32),
                pltpu.VMEM((CG_STEPS + 1, half_users, rank), F32),
                pltpu.VMEM((CG_STEPS + 1, NX - 1, half_users, rank), F32),
                pltpu.VMEM((CG_STEPS, users, rank), BF16),
                pltpu.VMEM((all_users, rank), BF16),
                pltpu.VMEM((rank, all_users), BF16),
                dma((2, NROW)),
                dma,
                dma((8,)),
                dma((CHUNKS, peers)),
                dma((CHUNKS, peers)),
                dma((CG_STEPS + 1,)),
                dma((CG_STEPS + 1,)),
                dma((CG_STEPS + 1, NX - 1)),
                dma((CG_STEPS + 1, NX - 1)),
                dma((CG_STEPS,)),
                dma((CG_STEPS,)),
                dma,
                dma,
                dma((peers,)),
                dma((peers,)),
                dma((NROW,)),
                dma((NROW,)),
                dma((CHUNKS, 2, 20)),
                dma((CHUNKS, 2, 20)),
            ],
            compiler_params=pltpu.CompilerParams(
                collective_id=0, has_side_effects=True, vmem_limit_bytes=48 * 2**20
            ),
            name="als_sweep",
        )(ratings, mask, user_init, item_init)

    return jax.shard_map(
        local_step,
        mesh=mesh,
        in_specs=(grid_spec, grid_spec, user_spec, item_spec),
        out_specs=(user_spec, item_spec),
        check_vma=False,
    )
```

```python
import jax
import jax.numpy as jnp
from jax import lax
from jax.experimental import pallas as pl
from jax.experimental.pallas import tpu as pltpu
from jax.sharding import PartitionSpec as P

CG_STEPS = 4
RIDGE_WEIGHT = 0.0005
MESH = pl.DeviceIdType.MESH
F32 = jnp.float32
BF16 = jnp.bfloat16

NZ = NY = 4
NROW = NZ * NY
NX = 4
NCOL = NX * 2
CHUNKS = 2
OFFSETS = [
    (1, 1), (3, 3), (1, 0), (3, 0), (2, 1), (2, 3), (2, 0), (1, 3), (3, 1), (1, 2), (3, 2), (2, 2), (0, 1), (0, 3), (0, 2),
]
NEAR_FIRST = sorted(
    range(len(OFFSETS)), key=lambda k: min(OFFSETS[k][0], NZ - OFFSETS[k][0]) + min(OFFSETS[k][1], NY - OFFSETS[k][1])
)
PACE = [(0, 1, 2), (3, 4, 5, 6), (7, 8, 9, 10), (), (11, 12, 13, 14)]


def dot(a, b, ca, cb):
    return lax.dot_general(a, b, (((ca,), (cb,)), ((), ())), preferred_element_type=F32)


def kernel(
    ratings, mask, user_init, item_init, user_out, item_out,
    r_in, m_in, v_in, w_in, fixed, fixed_t, mask_bf, r_send, r_recv, mask_items,
    masked, pair_send, pair_recv, chip_sum, x_recv, p_all, fw, fw_t,
    in_sem, w_in_sem, v_in_sem, a2a_send, a2a_recv, pair_send_sem, pair_recv_sem, x_send_sem, x_recv_sem,
    ag_send, ag_recv, wc_send, wc_recv, wr_send, wr_recv, wf_send, wf_recv, vg_send, vg_recv,
):
    users, items = r_in.shape
    rank = w_in.shape[1]
    half_users = users // 2
    own_items = items // NROW
    all_users = users * NROW
    width = own_items // CHUNKS
    half = width // 2
    tall = all_users // 4
    tile = items // 8
    row = lax.axis_index("row")
    col = lax.axis_index("col")
    zi = row // NY
    yi = lax.rem(row, NY)
    xi = col // 2
    core = lax.rem(col, 2)
    ridge_user = RIDGE_WEIGHT * items * NCOL
    ridge_item = RIDGE_WEIGHT * all_users
    partner = (0, row, xi * 2 + 1 - core)

    def row_of(dz, dy):
        return lax.rem(zi + dz, NZ) * NY + lax.rem(yi + dy, NY)

    def row_dev(r):
        return (0, r, col)

    def x_dev(k):
        return (0, row, lax.rem(xi + k, NX) * 2 + core)

    def remote(src, dst, send, recv, dev):
        return pltpu.make_async_remote_copy(
            src_ref=src, dst_ref=dst, send_sem=send, recv_sem=recv, device_id=dev, device_id_type=MESH
        )

    peers = [row_dev(row_of(dz, dy)) for dz, dy in OFFSETS] + [x_dev(k) for k in range(1, NX)] + [partner]
    barrier = pltpu.get_barrier_semaphore()
    for dev in peers:
        pl.semaphore_signal(barrier, inc=1, device_id=dev, device_id_type=MESH)

    order = OFFSETS + [(0, 0)]
    loads = []
    for k, (dz, dy) in enumerate(order):
        cols = pl.ds(pl.multiple_of(row_of(dz, dy) * own_items, own_items), own_items)
        a = pltpu.make_async_copy(ratings.at[:, cols], r_in.at[:, cols], in_sem.at[0, k])
        b = pltpu.make_async_copy(mask.at[:, cols], m_in.at[:, cols], in_sem.at[1, k])
        a.start()
        b.start()
        loads.append((a, b, cols))
    w_load = pltpu.make_async_copy(user_init, w_in, w_in_sem)
    w_load.start()
    v_loads = []
    for t in range(8):
        c = pltpu.make_async_copy(
            item_init.at[t * tile:(t + 1) * tile], v_in.at[t * tile:(t + 1) * tile], v_in_sem.at[t]
        )
        c.start()
        v_loads.append(c)

    my_users = pl.ds(pl.multiple_of(row * users, users), users)
    exchange = {}

    def exchange_start(k, q):
        dz, dy = order[k]
        c = remote(
            r_send.at[q, k], r_recv.at[q, my_users, :], a2a_send.at[q, k], a2a_recv.at[q, k],
            row_dev(row_of(dz, dy)),
        )
        c.start()
        exchange[q, k] = c

    ahead = 4
    for k, (dz, dy) in enumerate(order):
        a, b, cols = loads[k]
        a.wait()
        b.wait()
        on = m_in[:, cols] > 0
        mask_bf[:, cols] = on.astype(F32).astype(BF16)
        marked = jnp.where(on, r_in[:, cols], jnp.inf)
        for q in range(CHUNKS):
            if (dz, dy) == (0, 0):
                r_recv[q, my_users, :] = marked[:, q * width:(q + 1) * width]
            else:
                r_send[q, k] = marked[:, q * width:(q + 1) * width]
        if k == ahead - 1:
            pl.semaphore_wait(barrier, len(peers))
            for j in range(ahead):
                exchange_start(j, 0)
        elif k >= ahead and k < len(OFFSETS):
            exchange_start(k, 0)

    mine = pl.ds(pl.multiple_of(core * half_users, half_users), half_users)
    other = pl.ds(pl.multiple_of((1 - core) * half_users, half_users), half_users)
    sides = (other, mine)

    def reduce_users(it, product, meanwhile):
        pair_send[it] = product(0)
        c = remote(pair_send.at[it], pair_recv.at[it], pair_send_sem.at[it], pair_recv_sem.at[it], partner)
        c.start()
        chip_sum[it] = product(1)
        c.wait()
        own = chip_sum[it] + pair_recv[it]
        chip_sum[it] = own
        copies = []
        for k in (2, 1, 3):
            c = remote(
                chip_sum.at[it], x_recv.at[it, k - 1], x_send_sem.at[it, k - 1], x_recv_sem.at[it, k - 1], x_dev(k)
            )
            c.start()
            copies.append(c)
        meanwhile()
        for c in copies:
            c.wait()
        return (own + x_recv[it, 1]) + (x_recv[it, 0] + x_recv[it, 2])

    def share_direction(it, p):
        p_all[it, mine, :] = p.astype(BF16)
        c = remote(p_all.at[it, mine], p_all.at[it, mine], ag_send.at[it], ag_recv.at[it], partner)
        c.start()
        c.wait()

    def user_product(it):
        def product(side):
            rows = sides[side]
            p = p_all[it, rows, :]
            for t in range(8):
                cols = slice(t * tile, (t + 1) * tile)
                masked[side, :, cols] = dot(p, fixed_t[:, cols], 1, 0).astype(BF16) * mask_bf[rows, cols]
            return dot(masked[side], fixed[...], 1, 0)
        return product

    w_load.wait()
    w = w_in[...].astype(BF16)
    for t in range(8):
        cols = slice(t * tile, (t + 1) * tile)
        v_loads[t].wait()
        f = v_in[cols, :].astype(BF16)
        fixed[cols, :] = f
        d = jnp.where(m_in[:, cols] > 0, r_in[:, cols] - dot(w, f, 1, 1), 0.0).astype(BF16)
        masked[0, :, cols] = d[:half_users]
        masked[1, :, cols] = d[half_users:]

    def user_residual(side):
        return dot(masked[lax.rem(core + 1 + side, 2)], fixed[...], 1, 0)

    def item_mask(q):
        for k in range(len(OFFSETS)):
            exchange[q, k].wait()
        for t in range(4):
            rows = slice(t * tall, (t + 1) * tall)
            mask_items[q, rows, :] = jnp.where(r_recv[q, rows, :] < jnp.inf, 1.0, 0.0).astype(BF16)

    def meanwhile(it):
        def work():
            if it == 0:
                for t in range(8):
                    cols = slice(t * tile, (t + 1) * tile)
                    fixed_t[:, cols] = fixed[cols, :].T
            else:
                for k in PACE[it - 1]:
                    exchange_start(k, 1)
            if it == CG_STEPS:
                item_mask(0)
        return work

    x = w_in[mine, :]
    r = reduce_users(0, user_residual, meanwhile(0)) - ridge_user * x
    p = r
    rr = jnp.sum(r * r, axis=1, keepdims=True)
    share_direction(0, p)
    for it in range(1, CG_STEPS + 1):
        q = reduce_users(it, user_product(it - 1), meanwhile(it)) + ridge_user * p
        a = rr / jnp.sum(p * q, axis=1, keepdims=True)
        x = x + a * p
        if it < CG_STEPS:
            r = r - a * q
            rn = jnp.sum(r * r, axis=1, keepdims=True)
            p = r + (rn / rr) * p
            rr = rn
            share_direction(it, p)

    def user_block(r):
        return pl.ds(pl.multiple_of(r * users + core * half_users, half_users), half_users)

    fw[user_block(row), :] = x.astype(BF16)
    shared = {}
    for k in reversed(NEAR_FIRST):
        blk = user_block(row)
        c = remote(fw.at[blk], fw.at[blk], wr_send.at[k], wr_recv.at[k], row_dev(row_of(*OFFSETS[k])))
        c.start()
        shared[k] = c
    crossed = [remote(fw.at[user_block(row)], fw.at[user_block(row)], wf_send.at[NROW - 1], wf_recv.at[NROW - 1], partner)]
    crossed[0].start()
    user_out[mine, :] = x
    w_copy = remote(user_out.at[mine], user_out.at[mine], wc_send, wc_recv, partner)
    w_copy.start()

    for k in PACE[CG_STEPS]:
        exchange_start(k, 1)

    x_all = v_in[pl.ds(pl.multiple_of(row * own_items, own_items), own_items), :].T
    sources = [row]
    for k in NEAR_FIRST:
        shared[k].wait()
        src = row_of(NZ - OFFSETS[k][0], NY - OFFSETS[k][1])
        c = remote(fw.at[user_block(src)], fw.at[user_block(src)], wf_send.at[k], wf_recv.at[k], partner)
        c.start()
        crossed.append(c)
        sources.append(src)
    done = 0
    for n in (5, 6, 5):
        for c in crossed[done:done + n]:
            c.wait()
        for src in sources[done:done + n]:
            blk = pl.ds(pl.multiple_of(src * users, users), users)
            fw_t[:, blk] = fw[blk, :].T
        done += n

    def item_product(p_bf, q, first):
        acc = jnp.zeros((rank, width), F32)
        for t in range(4):
            rows = slice(t * tall, (t + 1) * tall)
            s = dot(fw[rows, :], p_bf, 1, 0)
            if first:
                known = r_recv[q, rows, :]
                z = jnp.where(known < jnp.inf, known - s, 0.0).astype(BF16)
            else:
                z = s.astype(BF16) * mask_items[q, rows, :]
            acc = acc + dot(fw_t[:, rows], z, 1, 0)
        return acc

    def block(r, q, h):
        return pl.ds(pl.multiple_of(r * own_items + q * width + h * half, half), half)

    def halfblock(r, q, h, part):
        n = half // 2
        return pl.ds(pl.multiple_of(r * own_items + q * width + h * half + part * n, n), n)

    dims = [((0, 1), (1, 0)), ((1, 0), (0, 1))]

    def scaled(d, n):
        return (d[0] * n % NZ, d[1] * n % NY)

    def added(d, e):
        return ((d[0] + e[0]) % NZ, (d[1] + e[1]) % NY)

    started = []

    def send(rows, dev, q, h, slot):
        c = remote(item_out.at[rows], item_out.at[rows], vg_send.at[q, h, slot], vg_recv.at[q, h, slot], dev)
        c.start()
        started.append(c)
        return c

    def gather_own(q):
        got = {}
        for h in range(2):
            d1, d2 = dims[h]
            for s, sign in enumerate((1, 3)):
                got[h, 0, s] = send(block(row, q, h), row_dev(row_of(*scaled(d1, sign))), q, h, s)
            for s, sign in enumerate((1, 3)):
                got[h, 1, 0, s] = send(block(row, q, h), row_dev(row_of(*scaled(d2, sign))), q, h, 4 + s)
        return got

    def gather_first(q, got):
        for s, sign in enumerate((1, 3)):
            for h in range(2):
                d1, d2 = dims[h]
                got[h, 0, s].wait_recv()
                src = row_of(*scaled(d1, 4 - sign))
                got[h, 2, s] = send(
                    halfblock(src, q, h, s), row_dev(row_of(*scaled(d1, sign))), q, h, 2 + s
                )
                for s2, sign2 in enumerate((1, 3)):
                    got[h, 1, 1 + s, s2] = send(
                        block(src, q, h), row_dev(row_of(*scaled(d2, sign2))), q, h, 6 + 2 * s + s2
                    )
        for h in range(2):
            d1, d2 = dims[h]
            got[h, 2, 0].wait_recv()
            got[h, 2, 1].wait_recv()
            src = row_of(*scaled(d1, 2))
            for s2, sign2 in enumerate((1, 3)):
                got[h, 1, 3, s2] = send(block(src, q, h), row_dev(row_of(*scaled(d2, sign2))), q, h, 10 + s2)

    def gather_second(q, got, b):
        for h in range(2):
            d1, d2 = dims[h]
            base = scaled(d1, (0, 3, 1, 2)[b])
            for s, sign in enumerate((1, 3)):
                got[h, 1, b, s].wait_recv()
                src = row_of(*added(base, scaled(d2, 4 - sign)))
                got[h, 3, b, s] = send(
                    halfblock(src, q, h, s), row_dev(row_of(*scaled(d2, sign))), q, h, 12 + 2 * b + s
                )

    pending = []
    for q in range(CHUNKS):
        if q:
            item_mask(q)
        x = x_all[:, q * width:(q + 1) * width]
        r = item_product(x.astype(BF16), q, True) - ridge_item * x
        p = r
        rr = jnp.sum(r * r, axis=0, keepdims=True)

        def item_step(_, state):
            x, r, p, rr = state
            g = item_product(p.astype(BF16), q, False) + ridge_item * p
            a = rr / jnp.sum(p * g, axis=0, keepdims=True)
            x = x + a * p
            r = r - a * g
            rn = jnp.sum(r * r, axis=0, keepdims=True)
            p = r + (rn / rr) * p
            return x, r, p, rn

        x, r, p, rr = lax.fori_loop(0, CG_STEPS - 1, item_step, (x, r, p, rr))
        g = item_product(p.astype(BF16), q, False) + ridge_item * p
        x = x + (rr / jnp.sum(p * g, axis=0, keepdims=True)) * p
        item_out[pl.ds(pl.multiple_of(row * own_items + q * width, width), width), :] = x.T
        pending.append(gather_own(q))

    for q in range(CHUNKS):
        gather_first(q, pending[q])
    for b in range(4):
        for q in range(CHUNKS):
            gather_second(q, pending[q], b)
    for q in range(CHUNKS):
        for h in range(2):
            for b in range(4):
                for s in range(2):
                    pending[q][h, 3, b, s].wait_recv()
    for c in started:
        c.wait_send()
    w_copy.wait()


def solution(mesh):
    grid_spec = P(("part", "row"), "col")
    user_spec = P(("part", "row"), None)
    item_spec = P(("part", "col"), None)

    def local_step(ratings, mask, user_init, item_init):
        users, items = ratings.shape
        rank = user_init.shape[1]
        own_items = items // NROW
        all_users = users * NROW
        width = own_items // CHUNKS
        half_users = users // 2
        peers = len(OFFSETS)
        dma = pltpu.SemaphoreType.DMA
        hbm = pl.BlockSpec(memory_space=pltpu.HBM)
        vmem = pl.BlockSpec(memory_space=pltpu.VMEM)
        return pl.pallas_call(
            kernel,
            out_shape=(pltpu.VMEM((users, rank), F32), pltpu.VMEM((items, rank), F32)),
            in_specs=[hbm] * 4,
            out_specs=(vmem, vmem),
            scratch_shapes=[
                pltpu.VMEM((users, items), F32),
                pltpu.VMEM((users, items), jnp.int32),
                pltpu.VMEM((items, rank), F32),
                pltpu.VMEM((users, rank), F32),
                pltpu.VMEM((items, rank), BF16),
                pltpu.VMEM((rank, items), BF16),
                pltpu.VMEM((users, items), BF16),
                pltpu.VMEM((CHUNKS, peers, users, width), F32),
                pltpu.VMEM((CHUNKS, all_users, width), F32),
                pltpu.VMEM((CHUNKS, all_users, width), BF16),
                pltpu.VMEM((2, half_users, items), BF16),
                pltpu.VMEM((CG_STEPS + 1, half_users, rank), F32),
                pltpu.VMEM((CG_STEPS + 1, half_users, rank), F32),
                pltpu.VMEM((CG_STEPS + 1, half_users, rank), F32),
                pltpu.VMEM((CG_STEPS + 1, NX - 1, half_users, rank), F32),
                pltpu.VMEM((CG_STEPS, users, rank), BF16),
                pltpu.VMEM((all_users, rank), BF16),
                pltpu.VMEM((rank, all_users), BF16),
                dma((2, NROW)),
                dma,
                dma((8,)),
                dma((CHUNKS, peers)),
                dma((CHUNKS, peers)),
                dma((CG_STEPS + 1,)),
                dma((CG_STEPS + 1,)),
                dma((CG_STEPS + 1, NX - 1)),
                dma((CG_STEPS + 1, NX - 1)),
                dma((CG_STEPS,)),
                dma((CG_STEPS,)),
                dma,
                dma,
                dma((peers,)),
                dma((peers,)),
                dma((NROW,)),
                dma((NROW,)),
                dma((CHUNKS, 2, 20)),
                dma((CHUNKS, 2, 20)),
            ],
            compiler_params=pltpu.CompilerParams(
                collective_id=0, has_side_effects=True, vmem_limit_bytes=48 * 2**20
            ),
            name="als_sweep",
        )(ratings, mask, user_init, item_init)

    return jax.shard_map(
        local_step,
        mesh=mesh,
        in_specs=(grid_spec, grid_spec, user_spec, item_spec),
        out_specs=(user_spec, item_spec),
        check_vma=False,
    )
```

```python
import jax
import jax.numpy as jnp
from jax import lax
from jax.experimental import pallas as pl
from jax.experimental.pallas import tpu as pltpu
from jax.sharding import PartitionSpec as P

CG_STEPS = 4
RIDGE_WEIGHT = 0.0005
MESH = pl.DeviceIdType.MESH
F32 = jnp.float32
BF16 = jnp.bfloat16

NZ = NY = 4
NROW = NZ * NY
NX = 4
NCOL = NX * 2
CHUNKS = 2
OFFSETS = [
    (1, 1), (3, 3), (3, 1), (1, 3), (0, 1), (2, 3), (2, 1), (0, 3), (2, 2), (1, 2), (3, 2), (0, 2), (1, 0), (3, 0), (2, 0),
]
NEAR_FIRST = sorted(
    range(len(OFFSETS)), key=lambda k: min(OFFSETS[k][0], NZ - OFFSETS[k][0]) + min(OFFSETS[k][1], NY - OFFSETS[k][1])
)
SLOT = {k: n + 1 for n, k in enumerate(NEAR_FIRST)}
PACE = [(), (), (0, 1, 2, 3), (4, 5, 6, 7), (8, 9, 10, 11, 12, 13, 14)]


def chunk_starts(own_items):
    return (0, own_items // 4, own_items)


def dot(a, b, ca, cb):
    return lax.dot_general(a, b, (((ca,), (cb,)), ((), ())), preferred_element_type=F32)


def kernel(
    ratings, mask, user_init, item_init, user_out, item_out,
    r_in, m_in, v_in, w_in, fixed, fixed_t, mask_bf, r_send0, r_send1, r_recv0, r_recv1, mask0, mask1, item_masked,
    masked, pair_send, pair_recv, chip_sum, x_recv, p_all, fw, fw_t, x_items,
    in_sem, w_in_sem, v_in_sem, a2a_send, a2a_recv, pair_send_sem, pair_recv_sem, x_send_sem, x_recv_sem,
    ag_send, ag_recv, wc_send, wc_recv, wr_send, wr_recv, wf_send, wf_recv, vg_send, vg_recv,
):
    users, items = r_in.shape
    rank = w_in.shape[1]
    half_users = users // 2
    own_items = items // NROW
    all_users = users * NROW
    starts = chunk_starts(own_items)
    widths = [starts[q + 1] - starts[q] for q in range(CHUNKS)]
    r_send, r_recv, mask_items = (r_send0, r_send1), (r_recv0, r_recv1), (mask0, mask1)
    tall = all_users // 4
    tile = items // 8
    row = lax.axis_index("row")
    col = lax.axis_index("col")
    zi = row // NY
    yi = lax.rem(row, NY)
    xi = col // 2
    core = lax.rem(col, 2)
    ridge_user = RIDGE_WEIGHT * items * NCOL
    ridge_item = RIDGE_WEIGHT * all_users
    partner = (0, row, xi * 2 + 1 - core)

    def row_of(dz, dy):
        return lax.rem(zi + dz, NZ) * NY + lax.rem(yi + dy, NY)

    def row_dev(r):
        return (0, r, col)

    def x_dev(k):
        return (0, row, lax.rem(xi + k, NX) * 2 + core)

    def remote(src, dst, send, recv, dev):
        return pltpu.make_async_remote_copy(
            src_ref=src, dst_ref=dst, send_sem=send, recv_sem=recv, device_id=dev, device_id_type=MESH
        )

    peers = [row_dev(row_of(dz, dy)) for dz, dy in OFFSETS] + [x_dev(k) for k in range(1, NX)] + [partner]
    barrier = pltpu.get_barrier_semaphore()
    for dev in peers:
        pl.semaphore_signal(barrier, inc=1, device_id=dev, device_id_type=MESH)

    order = OFFSETS + [(0, 0)]
    loads = []
    for k, (dz, dy) in enumerate(order):
        cols = pl.ds(pl.multiple_of(row_of(dz, dy) * own_items, own_items), own_items)
        a = pltpu.make_async_copy(ratings.at[:, cols], r_in.at[:, cols], in_sem.at[0, k])
        b = pltpu.make_async_copy(mask.at[:, cols], m_in.at[:, cols], in_sem.at[1, k])
        a.start()
        b.start()
        loads.append((a, b, cols))
    w_load = pltpu.make_async_copy(user_init, w_in, w_in_sem)
    w_load.start()
    v_loads = []
    for t in range(8):
        c = pltpu.make_async_copy(
            item_init.at[t * tile:(t + 1) * tile], v_in.at[t * tile:(t + 1) * tile], v_in_sem.at[t]
        )
        c.start()
        v_loads.append(c)

    exchange = {}

    def exchange_start(k, q, part):
        dz, dy = order[k]
        rows, n = ((0, users), (0, half_users), (half_users, half_users))[part]
        c = remote(
            r_send[q].at[k, pl.ds(rows, n)], r_recv[q].at[pl.ds(SLOT[k] * users + rows, n)],
            a2a_send.at[part, k], a2a_recv.at[part, k], row_dev(row_of(dz, dy)),
        )
        c.start()
        exchange[part, k] = c

    ahead = 4
    for k, (dz, dy) in enumerate(order):
        a, b, cols = loads[k]
        a.wait()
        b.wait()
        on = m_in[:, cols] > 0
        mask_bf[:, cols] = on.astype(F32).astype(BF16)
        marked = jnp.where(on, r_in[:, cols], jnp.inf)
        for q in range(CHUNKS):
            if (dz, dy) == (0, 0):
                r_recv[q][0:users, :] = marked[:, starts[q]:starts[q + 1]]
            else:
                r_send[q][k] = marked[:, starts[q]:starts[q + 1]]
        if k == ahead - 1:
            pl.semaphore_wait(barrier, len(peers))
            for j in range(ahead):
                exchange_start(j, 0, 0)
        elif k >= ahead and k < len(OFFSETS):
            exchange_start(k, 0, 0)
    for k in range(len(OFFSETS)):
        exchange_start(k, 1, 1)

    mine = pl.ds(pl.multiple_of(core * half_users, half_users), half_users)
    other = pl.ds(pl.multiple_of((1 - core) * half_users, half_users), half_users)
    sides = (other, mine)

    def reduce_users(it, product, meanwhile):
        pair_send[it] = product(0)
        c = remote(pair_send.at[it], pair_recv.at[it], pair_send_sem.at[it], pair_recv_sem.at[it], partner)
        c.start()
        chip_sum[it] = product(1)
        c.wait()
        own = chip_sum[it] + pair_recv[it]
        chip_sum[it] = own
        copies = []
        for k in (2, 1, 3):
            c = remote(
                chip_sum.at[it], x_recv.at[it, k - 1], x_send_sem.at[it, k - 1], x_recv_sem.at[it, k - 1], x_dev(k)
            )
            c.start()
            copies.append(c)
        meanwhile()
        for c in copies:
            c.wait()
        return (own + x_recv[it, 1]) + (x_recv[it, 0] + x_recv[it, 2])

    def share_direction(it, p):
        p_all[it, mine, :] = p.astype(BF16)
        c = remote(p_all.at[it, mine], p_all.at[it, mine], ag_send.at[it], ag_recv.at[it], partner)
        c.start()
        c.wait()

    def user_product(it):
        def product(side):
            rows = sides[side]
            p = p_all[it, rows, :]
            for t in range(8):
                cols = slice(t * tile, (t + 1) * tile)
                masked[side, :, cols] = dot(p, fixed_t[:, cols], 1, 0).astype(BF16) * mask_bf[rows, cols]
            return dot(masked[side], fixed[...], 1, 0)
        return product

    w_load.wait()
    w = w_in[...].astype(BF16)
    for t in range(8):
        cols = slice(t * tile, (t + 1) * tile)
        v_loads[t].wait()
        f = v_in[cols, :].astype(BF16)
        fixed[cols, :] = f
        d = jnp.where(m_in[:, cols] > 0, r_in[:, cols] - dot(w, f, 1, 1), 0.0).astype(BF16)
        masked[0, :, cols] = d[:half_users]
        masked[1, :, cols] = d[half_users:]

    def user_residual(side):
        return dot(masked[lax.rem(core + 1 + side, 2)], fixed[...], 1, 0)

    def item_mask(q):
        for part in (0,) if q == 0 else (1, 2):
            for k in range(len(OFFSETS)):
                exchange[part, k].wait()
        for t in range(4):
            rows = slice(t * tall, (t + 1) * tall)
            mask_items[q][rows, :] = jnp.where(r_recv[q][rows, :] < jnp.inf, 1.0, 0.0).astype(BF16)

    def meanwhile(it):
        def work():
            if it == 0:
                for t in range(8):
                    cols = slice(t * tile, (t + 1) * tile)
                    fixed_t[:, cols] = fixed[cols, :].T
            else:
                for k in PACE[it - 1]:
                    exchange_start(k, 1, 2)
            if it == 2:
                x_items[...] = v_in[pl.ds(pl.multiple_of(row * own_items, own_items), own_items), :].T
                item_mask(0)
        return work

    x = w_in[mine, :]
    r = reduce_users(0, user_residual, meanwhile(0)) - ridge_user * x
    p = r
    rr = jnp.sum(r * r, axis=1, keepdims=True)
    share_direction(0, p)
    for it in range(1, CG_STEPS + 1):
        q = reduce_users(it, user_product(it - 1), meanwhile(it)) + ridge_user * p
        a = rr / jnp.sum(p * q, axis=1, keepdims=True)
        x = x + a * p
        if it < CG_STEPS:
            r = r - a * q
            rn = jnp.sum(r * r, axis=1, keepdims=True)
            p = r + (rn / rr) * p
            rr = rn
            share_direction(it, p)

    def user_block(slot):
        return pl.ds(pl.multiple_of(slot * users + core * half_users, half_users), half_users)

    fw[user_block(0), :] = x.astype(BF16)
    shared = {}
    for k in reversed(NEAR_FIRST):
        c = remote(
            fw.at[user_block(0)], fw.at[user_block(SLOT[k])], wr_send.at[k], wr_recv.at[k],
            row_dev(row_of(*OFFSETS[k])),
        )
        c.start()
        shared[SLOT[k]] = c
    crossed = {}

    def cross(slot):
        blk = user_block(slot)
        crossed[slot] = remote(fw.at[blk], fw.at[blk], wf_send.at[slot], wf_recv.at[slot], partner)
        crossed[slot].start()

    cross(0)
    user_out[mine, :] = x
    w_copy = remote(user_out.at[mine], user_out.at[mine], wc_send, wc_recv, partner)
    w_copy.start()
    for k in PACE[CG_STEPS]:
        exchange_start(k, 1, 2)

    def arrive(t):
        for slot in range(4 * t, 4 * t + 4):
            if slot:
                shared[slot].wait()
                cross(slot)

    def settle(t):
        for slot in range(4 * t, 4 * t + 4):
            crossed[slot].wait()
        rows = slice(t * tall, (t + 1) * tall)
        fw_t[:, rows] = fw[rows, :].T

    def item_residual(p_bf, q, t):
        rows = slice(t * tall, (t + 1) * tall)
        known = r_recv[q][rows, :]
        z = jnp.where(known < jnp.inf, known - dot(fw[rows, :], p_bf, 1, 0), 0.0).astype(BF16)
        return dot(fw_t[:, rows], z, 1, 0)

    def item_product(p_bf, q):
        for t in range(4):
            rows = slice(t * tall, (t + 1) * tall)
            item_masked[rows, :widths[q]] = dot(fw[rows, :], p_bf, 1, 0).astype(BF16) * mask_items[q][rows, :]
        return dot(fw_t[...], item_masked[:, :widths[q]], 1, 0)

    def block(r, q, h):
        n = widths[q] // 2
        return pl.ds(pl.multiple_of(r * own_items + starts[q] + h * n, 64), n)

    def halfblock(r, q, h, part):
        n = widths[q] // 4
        return pl.ds(pl.multiple_of(r * own_items + starts[q] + (2 * h + part) * n, 32), n)

    dims = [((0, 1), (1, 0)), ((1, 0), (0, 1))]

    def scaled(d, n):
        return (d[0] * n % NZ, d[1] * n % NY)

    def added(d, e):
        return ((d[0] + e[0]) % NZ, (d[1] + e[1]) % NY)

    started = []

    def send(rows, dev, q, h, slot):
        c = remote(item_out.at[rows], item_out.at[rows], vg_send.at[q, h, slot], vg_recv.at[q, h, slot], dev)
        c.start()
        started.append(c)
        return c

    def gather_own(q):
        got = {}
        for h in range(2):
            d1, d2 = dims[h]
            for s, sign in enumerate((1, 3)):
                got[h, 0, s] = send(block(row, q, h), row_dev(row_of(*scaled(d1, sign))), q, h, s)
            for s, sign in enumerate((1, 3)):
                got[h, 1, 0, s] = send(block(row, q, h), row_dev(row_of(*scaled(d2, sign))), q, h, 4 + s)
        return got

    def gather_first(q, got):
        for s, sign in enumerate((1, 3)):
            for h in range(2):
                d1, d2 = dims[h]
                got[h, 0, s].wait_recv()
                src = row_of(*scaled(d1, 4 - sign))
                got[h, 2, s] = send(
                    halfblock(src, q, h, s), row_dev(row_of(*scaled(d1, sign))), q, h, 2 + s
                )
                for s2, sign2 in enumerate((1, 3)):
                    got[h, 1, 1 + s, s2] = send(
                        block(src, q, h), row_dev(row_of(*scaled(d2, sign2))), q, h, 6 + 2 * s + s2
                    )
        for h in range(2):
            d1, d2 = dims[h]
            got[h, 2, 0].wait_recv()
            got[h, 2, 1].wait_recv()
            src = row_of(*scaled(d1, 2))
            for s2, sign2 in enumerate((1, 3)):
                got[h, 1, 3, s2] = send(block(src, q, h), row_dev(row_of(*scaled(d2, sign2))), q, h, 10 + s2)

    def gather_second(q, got, b):
        for h in range(2):
            d1, d2 = dims[h]
            base = scaled(d1, (0, 3, 1, 2)[b])
            for s, sign in enumerate((1, 3)):
                got[h, 1, b, s].wait_recv()
                src = row_of(*added(base, scaled(d2, 4 - sign)))
                got[h, 3, b, s] = send(
                    halfblock(src, q, h, s), row_dev(row_of(*scaled(d2, sign))), q, h, 12 + 2 * b + s
                )

    pending = []
    for q in range(CHUNKS):
        if q:
            item_mask(q)
        x = x_items[:, starts[q]:starts[q + 1]]
        x_bf = x.astype(BF16)
        r = -ridge_item * x
        if q == 0:
            arrive(0)
            arrive(1)
        for t in range(4):
            if q == 0:
                settle(t)
            r = r + item_residual(x_bf, q, t)
            if q == 0 and t < 2:
                arrive(t + 2)
        p = r
        rr = jnp.sum(r * r, axis=0, keepdims=True)

        def item_step(_, state):
            x, r, p, rr = state
            g = item_product(p.astype(BF16), q) + ridge_item * p
            a = rr / jnp.sum(p * g, axis=0, keepdims=True)
            x = x + a * p
            r = r - a * g
            rn = jnp.sum(r * r, axis=0, keepdims=True)
            p = r + (rn / rr) * p
            return x, r, p, rn

        x, r, p, rr = lax.fori_loop(0, CG_STEPS - 1, item_step, (x, r, p, rr))
        g = item_product(p.astype(BF16), q) + ridge_item * p
        x = x + (rr / jnp.sum(p * g, axis=0, keepdims=True)) * p
        first = pl.multiple_of(row * own_items + starts[q], widths[0])
        item_out[pl.ds(first, widths[q]), :] = x.T
        pending.append(gather_own(q))

    for q in range(CHUNKS):
        gather_first(q, pending[q])
    for b in range(4):
        for q in range(CHUNKS):
            gather_second(q, pending[q], b)
    for q in range(CHUNKS):
        for h in range(2):
            for b in range(4):
                for s in range(2):
                    pending[q][h, 3, b, s].wait_recv()
    for c in started:
        c.wait_send()
    w_copy.wait()


def solution(mesh):
    grid_spec = P(("part", "row"), "col")
    user_spec = P(("part", "row"), None)
    item_spec = P(("part", "col"), None)

    def local_step(ratings, mask, user_init, item_init):
        users, items = ratings.shape
        rank = user_init.shape[1]
        own_items = items // NROW
        all_users = users * NROW
        starts = chunk_starts(own_items)
        widths = [starts[q + 1] - starts[q] for q in range(CHUNKS)]
        half_users = users // 2
        peers = len(OFFSETS)
        dma = pltpu.SemaphoreType.DMA
        hbm = pl.BlockSpec(memory_space=pltpu.HBM)
        vmem = pl.BlockSpec(memory_space=pltpu.VMEM)
        return pl.pallas_call(
            kernel,
            out_shape=(pltpu.VMEM((users, rank), F32), pltpu.VMEM((items, rank), F32)),
            in_specs=[hbm] * 4,
            out_specs=(vmem, vmem),
            scratch_shapes=[
                pltpu.VMEM((users, items), F32),
                pltpu.VMEM((users, items), jnp.int32),
                pltpu.VMEM((items, rank), F32),
                pltpu.VMEM((users, rank), F32),
                pltpu.VMEM((items, rank), BF16),
                pltpu.VMEM((rank, items), BF16),
                pltpu.VMEM((users, items), BF16),
                *[pltpu.VMEM((peers, users, w), F32) for w in widths],
                *[pltpu.VMEM((all_users, w), F32) for w in widths],
                *[pltpu.VMEM((all_users, w), BF16) for w in widths],
                pltpu.VMEM((all_users, widths[-1]), BF16),
                pltpu.VMEM((2, half_users, items), BF16),
                pltpu.VMEM((CG_STEPS + 1, half_users, rank), F32),
                pltpu.VMEM((CG_STEPS + 1, half_users, rank), F32),
                pltpu.VMEM((CG_STEPS + 1, half_users, rank), F32),
                pltpu.VMEM((CG_STEPS + 1, NX - 1, half_users, rank), F32),
                pltpu.VMEM((CG_STEPS, users, rank), BF16),
                pltpu.VMEM((all_users, rank), BF16),
                pltpu.VMEM((rank, all_users), BF16),
                pltpu.VMEM((rank, own_items), F32),
                dma((2, NROW)),
                dma,
                dma((8,)),
                dma((3, peers)),
                dma((3, peers)),
                dma((CG_STEPS + 1,)),
                dma((CG_STEPS + 1,)),
                dma((CG_STEPS + 1, NX - 1)),
                dma((CG_STEPS + 1, NX - 1)),
                dma((CG_STEPS,)),
                dma((CG_STEPS,)),
                dma,
                dma,
                dma((peers,)),
                dma((peers,)),
                dma((NROW,)),
                dma((NROW,)),
                dma((CHUNKS, 2, 20)),
                dma((CHUNKS, 2, 20)),
            ],
            compiler_params=pltpu.CompilerParams(
                collective_id=0, has_side_effects=True, vmem_limit_bytes=48 * 2**20
            ),
            name="als_sweep",
        )(ratings, mask, pltpu.with_memory_space_constraint(user_init, pltpu.HBM), item_init)

    return jax.shard_map(
        local_step,
        mesh=mesh,
        in_specs=(grid_spec, grid_spec, user_spec, item_spec),
        out_specs=(user_spec, item_spec),
        check_vma=False,
    )
```

```python
import jax
import jax.numpy as jnp
from jax import lax
from jax.experimental import pallas as pl
from jax.experimental.pallas import tpu as pltpu
from jax.sharding import PartitionSpec as P

CG_STEPS = 4
RIDGE_WEIGHT = 0.0005
MESH = pl.DeviceIdType.MESH
F32 = jnp.float32
BF16 = jnp.bfloat16

NZ = NY = 4
NROW = NZ * NY
NX = 4
NCOL = NX * 2
CHUNKS = 2
OFFSETS = [
    (1, 1), (3, 3), (3, 1), (1, 3), (0, 1), (2, 3), (2, 1), (0, 3), (2, 2), (1, 2), (3, 2), (0, 2), (1, 0), (3, 0), (2, 0),
]
NEAR_FIRST = sorted(
    range(len(OFFSETS)), key=lambda k: min(OFFSETS[k][0], NZ - OFFSETS[k][0]) + min(OFFSETS[k][1], NY - OFFSETS[k][1])
)
SLOT = {k: n + 1 for n, k in enumerate(NEAR_FIRST)}
PACE = [(), (), (), (), tuple(range(15))]


def chunk_starts(own_items):
    return (0, own_items * 3 // 4, own_items)


def dot(a, b, ca, cb):
    return lax.dot_general(a, b, (((ca,), (cb,)), ((), ())), preferred_element_type=F32)


def kernel(
    ratings, mask, user_init, item_init, user_out, item_out,
    r_in, m_in, v_in, w_in, fixed, fixed_t, mask_bf, r_send0, r_send1, r_recv0, r_recv1, mask0, mask1, item_masked,
    masked, pair_send, pair_recv, chip_sum, x_recv, p_all, fw, fw_t, x_items,
    in_sem, w_in_sem, v_in_sem, a2a_send, a2a_recv, pair_send_sem, pair_recv_sem, x_send_sem, x_recv_sem,
    ag_send, ag_recv, wc_send, wc_recv, wr_send, wr_recv, wf_send, wf_recv, vg_send, vg_recv,
):
    users, items = r_in.shape
    rank = w_in.shape[1]
    half_users = users // 2
    own_items = items // NROW
    all_users = users * NROW
    starts = chunk_starts(own_items)
    widths = [starts[q + 1] - starts[q] for q in range(CHUNKS)]
    r_send, r_recv, mask_items = (r_send0, r_send1), (r_recv0, r_recv1), (mask0, mask1)
    tall = all_users // 4
    tile = items // 8
    row = lax.axis_index("row")
    col = lax.axis_index("col")
    zi = row // NY
    yi = lax.rem(row, NY)
    xi = col // 2
    core = lax.rem(col, 2)
    ridge_user = RIDGE_WEIGHT * items * NCOL
    ridge_item = RIDGE_WEIGHT * all_users
    partner = (0, row, xi * 2 + 1 - core)

    def row_of(dz, dy):
        return lax.rem(zi + dz, NZ) * NY + lax.rem(yi + dy, NY)

    def row_dev(r):
        return (0, r, col)

    def x_dev(k):
        return (0, row, lax.rem(xi + k, NX) * 2 + core)

    def remote(src, dst, send, recv, dev):
        return pltpu.make_async_remote_copy(
            src_ref=src, dst_ref=dst, send_sem=send, recv_sem=recv, device_id=dev, device_id_type=MESH
        )

    peers = [row_dev(row_of(dz, dy)) for dz, dy in OFFSETS] + [x_dev(k) for k in range(1, NX)] + [partner]
    barrier = pltpu.get_barrier_semaphore()
    for dev in peers:
        pl.semaphore_signal(barrier, inc=1, device_id=dev, device_id_type=MESH)

    order = OFFSETS + [(0, 0)]
    loads = []
    for k, (dz, dy) in enumerate(order):
        cols = pl.ds(pl.multiple_of(row_of(dz, dy) * own_items, own_items), own_items)
        a = pltpu.make_async_copy(ratings.at[:, cols], r_in.at[:, cols], in_sem.at[0, k])
        b = pltpu.make_async_copy(mask.at[:, cols], m_in.at[:, cols], in_sem.at[1, k])
        a.start()
        b.start()
        loads.append((a, b, cols))
    w_load = pltpu.make_async_copy(user_init, w_in, w_in_sem)
    w_load.start()
    v_loads = []
    for t in range(8):
        c = pltpu.make_async_copy(
            item_init.at[t * tile:(t + 1) * tile], v_in.at[t * tile:(t + 1) * tile], v_in_sem.at[t]
        )
        c.start()
        v_loads.append(c)

    exchange = {}

    def exchange_start(k, q):
        dz, dy = order[k]
        c = remote(
            r_send[q].at[k], r_recv[q].at[pl.ds(SLOT[k] * users, users)],
            a2a_send.at[q, k], a2a_recv.at[q, k], row_dev(row_of(dz, dy)),
        )
        c.start()
        exchange[q, k] = c

    ahead = 4
    for k, (dz, dy) in enumerate(order):
        a, b, cols = loads[k]
        a.wait()
        b.wait()
        on = m_in[:, cols] > 0
        mask_bf[:, cols] = on.astype(F32).astype(BF16)
        marked = jnp.where(on, r_in[:, cols], jnp.inf)
        for q in range(CHUNKS):
            if (dz, dy) == (0, 0):
                r_recv[q][0:users, :] = marked[:, starts[q]:starts[q + 1]]
            else:
                r_send[q][k] = marked[:, starts[q]:starts[q + 1]]
        if k == ahead - 1:
            pl.semaphore_wait(barrier, len(peers))
            for j in range(ahead):
                exchange_start(j, 0)
        elif k >= ahead and k < len(OFFSETS):
            exchange_start(k, 0)

    mine = pl.ds(pl.multiple_of(core * half_users, half_users), half_users)
    other = pl.ds(pl.multiple_of((1 - core) * half_users, half_users), half_users)
    sides = (other, mine)

    def reduce_users(it, product, meanwhile):
        pair_send[it] = product(0)
        c = remote(pair_send.at[it], pair_recv.at[it], pair_send_sem.at[it], pair_recv_sem.at[it], partner)
        c.start()
        chip_sum[it] = product(1)
        c.wait()
        own = chip_sum[it] + pair_recv[it]
        chip_sum[it] = own
        copies = []
        for k in (2, 1, 3):
            c = remote(
                chip_sum.at[it], x_recv.at[it, k - 1], x_send_sem.at[it, k - 1], x_recv_sem.at[it, k - 1], x_dev(k)
            )
            c.start()
            copies.append(c)
        meanwhile()
        for c in copies:
            c.wait()
        return (own + x_recv[it, 1]) + (x_recv[it, 0] + x_recv[it, 2])

    def share_direction(it, p):
        p_all[it, mine, :] = p.astype(BF16)
        c = remote(p_all.at[it, mine], p_all.at[it, mine], ag_send.at[it], ag_recv.at[it], partner)
        c.start()
        c.wait()

    def user_product(it):
        def product(side):
            rows = sides[side]
            p = p_all[it, rows, :]
            for t in range(8):
                cols = slice(t * tile, (t + 1) * tile)
                masked[side, :, cols] = dot(p, fixed_t[:, cols], 1, 0).astype(BF16) * mask_bf[rows, cols]
            return dot(masked[side], fixed[...], 1, 0)
        return product

    w_load.wait()
    w = w_in[...].astype(BF16)
    for t in range(8):
        cols = slice(t * tile, (t + 1) * tile)
        v_loads[t].wait()
        f = v_in[cols, :].astype(BF16)
        fixed[cols, :] = f
        d = jnp.where(m_in[:, cols] > 0, r_in[:, cols] - dot(w, f, 1, 1), 0.0).astype(BF16)
        masked[0, :, cols] = d[:half_users]
        masked[1, :, cols] = d[half_users:]

    def user_residual(side):
        return dot(masked[lax.rem(core + 1 + side, 2)], fixed[...], 1, 0)

    def item_mask(q):
        for k in range(len(OFFSETS)):
            exchange[q, k].wait()
        for t in range(4):
            rows = slice(t * tall, (t + 1) * tall)
            mask_items[q][rows, :] = jnp.where(r_recv[q][rows, :] < jnp.inf, 1.0, 0.0).astype(BF16)

    def meanwhile(it):
        def work():
            if it == 0:
                for t in range(8):
                    cols = slice(t * tile, (t + 1) * tile)
                    fixed_t[:, cols] = fixed[cols, :].T
            else:
                for k in PACE[it - 1]:
                    exchange_start(k, 1)
            if it == CG_STEPS:
                x_items[...] = v_in[pl.ds(pl.multiple_of(row * own_items, own_items), own_items), :].T
                item_mask(0)
        return work

    x = w_in[mine, :]
    r = reduce_users(0, user_residual, meanwhile(0)) - ridge_user * x
    p = r
    rr = jnp.sum(r * r, axis=1, keepdims=True)
    share_direction(0, p)
    for it in range(1, CG_STEPS + 1):
        q = reduce_users(it, user_product(it - 1), meanwhile(it)) + ridge_user * p
        a = rr / jnp.sum(p * q, axis=1, keepdims=True)
        x = x + a * p
        if it < CG_STEPS:
            r = r - a * q
            rn = jnp.sum(r * r, axis=1, keepdims=True)
            p = r + (rn / rr) * p
            rr = rn
            share_direction(it, p)

    def user_block(slot):
        return pl.ds(pl.multiple_of(slot * users + core * half_users, half_users), half_users)

    fw[user_block(0), :] = x.astype(BF16)
    shared = {}
    for k in reversed(NEAR_FIRST):
        c = remote(
            fw.at[user_block(0)], fw.at[user_block(SLOT[k])], wr_send.at[k], wr_recv.at[k],
            row_dev(row_of(*OFFSETS[k])),
        )
        c.start()
        shared[SLOT[k]] = c
    crossed = {}

    def cross(slot):
        blk = user_block(slot)
        crossed[slot] = remote(fw.at[blk], fw.at[blk], wf_send.at[slot], wf_recv.at[slot], partner)
        crossed[slot].start()

    cross(0)
    user_out[mine, :] = x
    w_copy = remote(user_out.at[mine], user_out.at[mine], wc_send, wc_recv, partner)
    w_copy.start()
    for k in PACE[CG_STEPS]:
        exchange_start(k, 1)

    def arrive(t):
        for slot in range(4 * t, 4 * t + 4):
            if slot:
                shared[slot].wait()
                cross(slot)

    def settle(t):
        for slot in range(4 * t, 4 * t + 4):
            crossed[slot].wait()
        rows = slice(t * tall, (t + 1) * tall)
        fw_t[:, rows] = fw[rows, :].T

    def item_residual(p_bf, q, t):
        rows = slice(t * tall, (t + 1) * tall)
        known = r_recv[q][rows, :]
        z = jnp.where(known < jnp.inf, known - dot(fw[rows, :], p_bf, 1, 0), 0.0).astype(BF16)
        return dot(fw_t[:, rows], z, 1, 0)

    def item_product(p_bf, q):
        for t in range(4):
            rows = slice(t * tall, (t + 1) * tall)
            item_masked[rows, :widths[q]] = dot(fw[rows, :], p_bf, 1, 0).astype(BF16) * mask_items[q][rows, :]
        return dot(fw_t[...], item_masked[:, :widths[q]], 1, 0)

    def block(r, q, h):
        n = widths[q] // 2
        return pl.ds(pl.multiple_of(r * own_items + starts[q] + h * n, 64), n)

    def halfblock(r, q, h, part):
        n = widths[q] // 4
        return pl.ds(pl.multiple_of(r * own_items + starts[q] + (2 * h + part) * n, 32), n)

    dims = [((0, 1), (1, 0)), ((1, 0), (0, 1))]

    def scaled(d, n):
        return (d[0] * n % NZ, d[1] * n % NY)

    def added(d, e):
        return ((d[0] + e[0]) % NZ, (d[1] + e[1]) % NY)

    started = []

    def send(rows, dev, q, h, slot):
        c = remote(item_out.at[rows], item_out.at[rows], vg_send.at[q, h, slot], vg_recv.at[q, h, slot], dev)
        c.start()
        started.append(c)
        return c

    def gather_own(q):
        got = {}
        for h in range(2):
            d1, d2 = dims[h]
            for s, sign in enumerate((1, 3)):
                got[h, 0, s] = send(block(row, q, h), row_dev(row_of(*scaled(d1, sign))), q, h, s)
            for s, sign in enumerate((1, 3)):
                got[h, 1, 0, s] = send(block(row, q, h), row_dev(row_of(*scaled(d2, sign))), q, h, 4 + s)
        return got

    def gather_first(q, got):
        for s, sign in enumerate((1, 3)):
            for h in range(2):
                d1, d2 = dims[h]
                got[h, 0, s].wait_recv()
                src = row_of(*scaled(d1, 4 - sign))
                got[h, 2, s] = send(
                    halfblock(src, q, h, s), row_dev(row_of(*scaled(d1, sign))), q, h, 2 + s
                )
                for s2, sign2 in enumerate((1, 3)):
                    got[h, 1, 1 + s, s2] = send(
                        block(src, q, h), row_dev(row_of(*scaled(d2, sign2))), q, h, 6 + 2 * s + s2
                    )
        for h in range(2):
            d1, d2 = dims[h]
            got[h, 2, 0].wait_recv()
            got[h, 2, 1].wait_recv()
            src = row_of(*scaled(d1, 2))
            for s2, sign2 in enumerate((1, 3)):
                got[h, 1, 3, s2] = send(block(src, q, h), row_dev(row_of(*scaled(d2, sign2))), q, h, 10 + s2)

    def gather_second(q, got, b):
        for h in range(2):
            d1, d2 = dims[h]
            base = scaled(d1, (0, 3, 1, 2)[b])
            for s, sign in enumerate((1, 3)):
                got[h, 1, b, s].wait_recv()
                src = row_of(*added(base, scaled(d2, 4 - sign)))
                got[h, 3, b, s] = send(
                    halfblock(src, q, h, s), row_dev(row_of(*scaled(d2, sign))), q, h, 12 + 2 * b + s
                )

    pending = []
    for q in range(CHUNKS):
        if q:
            item_mask(q)
        x = x_items[:, starts[q]:starts[q + 1]]
        x_bf = x.astype(BF16)
        r = -ridge_item * x
        if q == 0:
            arrive(0)
            arrive(1)
        for t in range(4):
            if q == 0:
                settle(t)
            r = r + item_residual(x_bf, q, t)
            if q == 0 and t < 2:
                arrive(t + 2)
        p = r
        rr = jnp.sum(r * r, axis=0, keepdims=True)

        def item_step(_, state):
            x, r, p, rr = state
            g = item_product(p.astype(BF16), q) + ridge_item * p
            a = rr / jnp.sum(p * g, axis=0, keepdims=True)
            x = x + a * p
            r = r - a * g
            rn = jnp.sum(r * r, axis=0, keepdims=True)
            p = r + (rn / rr) * p
            return x, r, p, rn

        x, r, p, rr = lax.fori_loop(0, CG_STEPS - 1, item_step, (x, r, p, rr))
        g = item_product(p.astype(BF16), q) + ridge_item * p
        x = x + (rr / jnp.sum(p * g, axis=0, keepdims=True)) * p
        first = pl.multiple_of(row * own_items + starts[q], 128)
        item_out[pl.ds(first, widths[q]), :] = x.T
        pending.append(gather_own(q))

    for q in range(CHUNKS):
        gather_first(q, pending[q])
    for b in range(4):
        for q in range(CHUNKS):
            gather_second(q, pending[q], b)
    for q in range(CHUNKS):
        for h in range(2):
            for b in range(4):
                for s in range(2):
                    pending[q][h, 3, b, s].wait_recv()
    for c in started:
        c.wait_send()
    w_copy.wait()


def solution(mesh):
    grid_spec = P(("part", "row"), "col")
    user_spec = P(("part", "row"), None)
    item_spec = P(("part", "col"), None)

    def local_step(ratings, mask, user_init, item_init):
        users, items = ratings.shape
        rank = user_init.shape[1]
        own_items = items // NROW
        all_users = users * NROW
        starts = chunk_starts(own_items)
        widths = [starts[q + 1] - starts[q] for q in range(CHUNKS)]
        half_users = users // 2
        peers = len(OFFSETS)
        dma = pltpu.SemaphoreType.DMA
        hbm = pl.BlockSpec(memory_space=pltpu.HBM)
        vmem = pl.BlockSpec(memory_space=pltpu.VMEM)
        return pl.pallas_call(
            kernel,
            out_shape=(pltpu.VMEM((users, rank), F32), pltpu.VMEM((items, rank), F32)),
            in_specs=[hbm] * 4,
            out_specs=(vmem, vmem),
            scratch_shapes=[
                pltpu.VMEM((users, items), F32),
                pltpu.VMEM((users, items), jnp.int32),
                pltpu.VMEM((items, rank), F32),
                pltpu.VMEM((users, rank), F32),
                pltpu.VMEM((items, rank), BF16),
                pltpu.VMEM((rank, items), BF16),
                pltpu.VMEM((users, items), BF16),
                *[pltpu.VMEM((peers, users, w), F32) for w in widths],
                *[pltpu.VMEM((all_users, w), F32) for w in widths],
                *[pltpu.VMEM((all_users, w), BF16) for w in widths],
                pltpu.VMEM((all_users, max(widths)), BF16),
                pltpu.VMEM((2, half_users, items), BF16),
                pltpu.VMEM((CG_STEPS + 1, half_users, rank), F32),
                pltpu.VMEM((CG_STEPS + 1, half_users, rank), F32),
                pltpu.VMEM((CG_STEPS + 1, half_users, rank), F32),
                pltpu.VMEM((CG_STEPS + 1, NX - 1, half_users, rank), F32),
                pltpu.VMEM((CG_STEPS, users, rank), BF16),
                pltpu.VMEM((all_users, rank), BF16),
                pltpu.VMEM((rank, all_users), BF16),
                pltpu.VMEM((rank, own_items), F32),
                dma((2, NROW)),
                dma,
                dma((8,)),
                dma((CHUNKS, peers)),
                dma((CHUNKS, peers)),
                dma((CG_STEPS + 1,)),
                dma((CG_STEPS + 1,)),
                dma((CG_STEPS + 1, NX - 1)),
                dma((CG_STEPS + 1, NX - 1)),
                dma((CG_STEPS,)),
                dma((CG_STEPS,)),
                dma,
                dma,
                dma((peers,)),
                dma((peers,)),
                dma((NROW,)),
                dma((NROW,)),
                dma((CHUNKS, 2, 20)),
                dma((CHUNKS, 2, 20)),
            ],
            compiler_params=pltpu.CompilerParams(
                collective_id=0, has_side_effects=True, vmem_limit_bytes=48 * 2**20
            ),
            name="als_sweep",
        )(ratings, mask, pltpu.with_memory_space_constraint(user_init, pltpu.HBM), item_init)

    return jax.shard_map(
        local_step,
        mesh=mesh,
        in_specs=(grid_spec, grid_spec, user_spec, item_spec),
        out_specs=(user_spec, item_spec),
        check_vma=False,
    )
```

```python
import jax
import jax.numpy as jnp
from jax import lax
from jax.experimental import pallas as pl
from jax.experimental.pallas import tpu as pltpu
from jax.sharding import PartitionSpec as P

CG_STEPS = 4
RIDGE_WEIGHT = 0.0005
MESH = pl.DeviceIdType.MESH
F32 = jnp.float32
BF16 = jnp.bfloat16

NZ = NY = 4
NROW = NZ * NY
NX = 4
NCOL = NX * 2
CHUNKS = 2
OFFSETS = [
    (1, 1), (3, 3), (1, 0), (3, 0), (2, 1), (2, 3), (2, 0), (1, 3), (3, 1), (1, 2), (3, 2), (2, 2), (0, 1), (0, 3), (0, 2),
]
NEAR_FIRST = sorted(
    range(len(OFFSETS)), key=lambda k: min(OFFSETS[k][0], NZ - OFFSETS[k][0]) + min(OFFSETS[k][1], NY - OFFSETS[k][1])
)
SLOT = {k: n + 1 for n, k in enumerate(NEAR_FIRST)}
PACE = [(), (), (), (), tuple(range(15))]


def chunk_starts(own_items):
    return (0, own_items * 3 // 4, own_items)


def dot(a, b, ca, cb):
    return lax.dot_general(a, b, (((ca,), (cb,)), ((), ())), preferred_element_type=F32)


def kernel(
    ratings, mask, user_init, item_init, user_out, item_out,
    r_in, m_in, v_in, w_in, fixed, fixed_t, mask_bf, r_send0, r_send1, r_recv0, r_recv1, mask0, mask1, item_masked,
    masked, pair_send, pair_recv, chip_sum, x_recv, p_all, fw, fw_t, x_items,
    in_sem, w_in_sem, v_in_sem, a2a_send, a2a_recv, pair_send_sem, pair_recv_sem, x_send_sem, x_recv_sem,
    ag_send, ag_recv, wc_send, wc_recv, wr_send, wr_recv, wf_send, wf_recv, vg_send, vg_recv,
):
    users, items = r_in.shape
    rank = w_in.shape[1]
    half_users = users // 2
    own_items = items // NROW
    all_users = users * NROW
    starts = chunk_starts(own_items)
    widths = [starts[q + 1] - starts[q] for q in range(CHUNKS)]
    r_send, r_recv, mask_items = (r_send0, r_send1), (r_recv0, r_recv1), (mask0, mask1)
    tall = all_users // 4
    tile = items // 8
    row = lax.axis_index("row")
    col = lax.axis_index("col")
    zi = row // NY
    yi = lax.rem(row, NY)
    xi = col // 2
    core = lax.rem(col, 2)
    ridge_user = RIDGE_WEIGHT * items * NCOL
    ridge_item = RIDGE_WEIGHT * all_users
    partner = (0, row, xi * 2 + 1 - core)

    def row_of(dz, dy):
        return lax.rem(zi + dz, NZ) * NY + lax.rem(yi + dy, NY)

    def row_dev(r):
        return (0, r, col)

    def x_dev(k):
        return (0, row, lax.rem(xi + k, NX) * 2 + core)

    def remote(src, dst, send, recv, dev):
        return pltpu.make_async_remote_copy(
            src_ref=src, dst_ref=dst, send_sem=send, recv_sem=recv, device_id=dev, device_id_type=MESH
        )

    peers = [row_dev(row_of(dz, dy)) for dz, dy in OFFSETS] + [x_dev(k) for k in range(1, NX)] + [partner]
    barrier = pltpu.get_barrier_semaphore()
    for dev in peers:
        pl.semaphore_signal(barrier, inc=1, device_id=dev, device_id_type=MESH)

    order = OFFSETS + [(0, 0)]
    loads = []
    for k, (dz, dy) in enumerate(order):
        cols = pl.ds(pl.multiple_of(row_of(dz, dy) * own_items, own_items), own_items)
        a = pltpu.make_async_copy(ratings.at[:, cols], r_in.at[:, cols], in_sem.at[0, k])
        b = pltpu.make_async_copy(mask.at[:, cols], m_in.at[:, cols], in_sem.at[1, k])
        a.start()
        b.start()
        loads.append((a, b, cols))
    w_load = pltpu.make_async_copy(user_init, w_in, w_in_sem)
    w_load.start()
    v_loads = []
    for t in range(8):
        c = pltpu.make_async_copy(
            item_init.at[t * tile:(t + 1) * tile], v_in.at[t * tile:(t + 1) * tile], v_in_sem.at[t]
        )
        c.start()
        v_loads.append(c)

    exchange = {}

    def exchange_start(k, q):
        dz, dy = order[k]
        c = remote(
            r_send[q].at[k], r_recv[q].at[pl.ds(SLOT[k] * users, users)],
            a2a_send.at[q, k], a2a_recv.at[q, k], row_dev(row_of(dz, dy)),
        )
        c.start()
        exchange[q, k] = c

    ahead = 4
    for k, (dz, dy) in enumerate(order):
        a, b, cols = loads[k]
        a.wait()
        b.wait()
        on = m_in[:, cols] > 0
        mask_bf[:, cols] = on.astype(F32).astype(BF16)
        marked = jnp.where(on, r_in[:, cols], jnp.inf)
        for q in range(CHUNKS):
            if (dz, dy) == (0, 0):
                r_recv[q][0:users, :] = marked[:, starts[q]:starts[q + 1]]
            else:
                r_send[q][k] = marked[:, starts[q]:starts[q + 1]]
        if k == ahead - 1:
            pl.semaphore_wait(barrier, len(peers))
            for j in range(ahead):
                exchange_start(j, 0)
        elif k >= ahead and k < len(OFFSETS):
            exchange_start(k, 0)

    mine = pl.ds(pl.multiple_of(core * half_users, half_users), half_users)
    other = pl.ds(pl.multiple_of((1 - core) * half_users, half_users), half_users)
    sides = (other, mine)

    def reduce_users(it, product, meanwhile):
        pair_send[it] = product(0)
        c = remote(pair_send.at[it], pair_recv.at[it], pair_send_sem.at[it], pair_recv_sem.at[it], partner)
        c.start()
        chip_sum[it] = product(1)
        c.wait()
        own = chip_sum[it] + pair_recv[it]
        chip_sum[it] = own
        copies = []
        for k in (2, 1, 3):
            c = remote(
                chip_sum.at[it], x_recv.at[it, k - 1], x_send_sem.at[it, k - 1], x_recv_sem.at[it, k - 1], x_dev(k)
            )
            c.start()
            copies.append(c)
        meanwhile()
        for c in copies:
            c.wait()
        return (own + x_recv[it, 1]) + (x_recv[it, 0] + x_recv[it, 2])

    def share_direction(it, p):
        p_all[it, mine, :] = p.astype(BF16)
        c = remote(p_all.at[it, mine], p_all.at[it, mine], ag_send.at[it], ag_recv.at[it], partner)
        c.start()
        c.wait()

    def user_product(it):
        def product(side):
            rows = sides[side]
            p = p_all[it, rows, :]
            for t in range(8):
                cols = slice(t * tile, (t + 1) * tile)
                masked[side, :, cols] = dot(p, fixed_t[:, cols], 1, 0).astype(BF16) * mask_bf[rows, cols]
            return dot(masked[side], fixed[...], 1, 0)
        return product

    w_load.wait()
    w = w_in[...].astype(BF16)
    for t in range(8):
        cols = slice(t * tile, (t + 1) * tile)
        v_loads[t].wait()
        f = v_in[cols, :].astype(BF16)
        fixed[cols, :] = f
        d = jnp.where(m_in[:, cols] > 0, r_in[:, cols] - dot(w, f, 1, 1), 0.0).astype(BF16)
        masked[0, :, cols] = d[:half_users]
        masked[1, :, cols] = d[half_users:]

    def user_residual(side):
        return dot(masked[lax.rem(core + 1 + side, 2)], fixed[...], 1, 0)

    def item_mask(q):
        for k in range(len(OFFSETS)):
            exchange[q, k].wait()
        for t in range(4):
            rows = slice(t * tall, (t + 1) * tall)
            mask_items[q][rows, :] = jnp.where(r_recv[q][rows, :] < jnp.inf, 1.0, 0.0).astype(BF16)

    def meanwhile(it):
        def work():
            if it == 0:
                for t in range(8):
                    cols = slice(t * tile, (t + 1) * tile)
                    fixed_t[:, cols] = fixed[cols, :].T
            else:
                for k in PACE[it - 1]:
                    exchange_start(k, 1)
            if it == CG_STEPS:
                x_items[...] = v_in[pl.ds(pl.multiple_of(row * own_items, own_items), own_items), :].T
                item_mask(0)
        return work

    x = w_in[mine, :]
    r = reduce_users(0, user_residual, meanwhile(0)) - ridge_user * x
    p = r
    rr = jnp.sum(r * r, axis=1, keepdims=True)
    share_direction(0, p)
    for it in range(1, CG_STEPS + 1):
        q = reduce_users(it, user_product(it - 1), meanwhile(it)) + ridge_user * p
        a = rr / jnp.sum(p * q, axis=1, keepdims=True)
        x = x + a * p
        if it < CG_STEPS:
            r = r - a * q
            rn = jnp.sum(r * r, axis=1, keepdims=True)
            p = r + (rn / rr) * p
            rr = rn
            share_direction(it, p)

    def user_block(slot):
        return pl.ds(pl.multiple_of(slot * users + core * half_users, half_users), half_users)

    fw[user_block(0), :] = x.astype(BF16)
    shared = {}
    for k in reversed(NEAR_FIRST):
        c = remote(
            fw.at[user_block(0)], fw.at[user_block(SLOT[k])], wr_send.at[k], wr_recv.at[k],
            row_dev(row_of(*OFFSETS[k])),
        )
        c.start()
        shared[SLOT[k]] = c
    crossed = {}

    def cross(slot):
        blk = user_block(slot)
        crossed[slot] = remote(fw.at[blk], fw.at[blk], wf_send.at[slot], wf_recv.at[slot], partner)
        crossed[slot].start()

    cross(0)
    user_out[mine, :] = x
    w_copy = remote(user_out.at[mine], user_out.at[mine], wc_send, wc_recv, partner)
    w_copy.start()
    for k in PACE[CG_STEPS]:
        exchange_start(k, 1)

    def arrive(t):
        for slot in range(4 * t, 4 * t + 4):
            if slot:
                shared[slot].wait()
                cross(slot)

    def settle(t):
        for slot in range(4 * t, 4 * t + 4):
            crossed[slot].wait()
        rows = slice(t * tall, (t + 1) * tall)
        fw_t[:, rows] = fw[rows, :].T

    def item_residual(p_bf, q, t):
        rows = slice(t * tall, (t + 1) * tall)
        known = r_recv[q][rows, :]
        z = jnp.where(known < jnp.inf, known - dot(fw[rows, :], p_bf, 1, 0), 0.0).astype(BF16)
        return dot(fw_t[:, rows], z, 1, 0)

    def item_product(p_bf, q):
        for t in range(4):
            rows = slice(t * tall, (t + 1) * tall)
            item_masked[rows, :widths[q]] = dot(fw[rows, :], p_bf, 1, 0).astype(BF16) * mask_items[q][rows, :]
        return dot(fw_t[...], item_masked[:, :widths[q]], 1, 0)

    def block(r, q, h):
        n = widths[q] // 2
        return pl.ds(pl.multiple_of(r * own_items + starts[q] + h * n, 64), n)

    def halfblock(r, q, h, part):
        n = widths[q] // 4
        return pl.ds(pl.multiple_of(r * own_items + starts[q] + (2 * h + part) * n, 32), n)

    dims = [((0, 1), (1, 0)), ((1, 0), (0, 1))]

    def scaled(d, n):
        return (d[0] * n % NZ, d[1] * n % NY)

    def added(d, e):
        return ((d[0] + e[0]) % NZ, (d[1] + e[1]) % NY)

    started = []

    def send(rows, dev, q, h, slot):
        c = remote(item_out.at[rows], item_out.at[rows], vg_send.at[q, h, slot], vg_recv.at[q, h, slot], dev)
        c.start()
        started.append(c)
        return c

    def gather_own(q):
        got = {}
        for h in range(2):
            d1, d2 = dims[h]
            for s, sign in enumerate((1, 3)):
                got[h, 0, s] = send(block(row, q, h), row_dev(row_of(*scaled(d1, sign))), q, h, s)
            for s, sign in enumerate((1, 3)):
                got[h, 1, 0, s] = send(block(row, q, h), row_dev(row_of(*scaled(d2, sign))), q, h, 4 + s)
        return got

    def gather_first(q, got):
        for s, sign in enumerate((1, 3)):
            for h in range(2):
                d1, d2 = dims[h]
                got[h, 0, s].wait_recv()
                src = row_of(*scaled(d1, 4 - sign))
                got[h, 2, s] = send(
                    halfblock(src, q, h, s), row_dev(row_of(*scaled(d1, sign))), q, h, 2 + s
                )
                for s2, sign2 in enumerate((1, 3)):
                    got[h, 1, 1 + s, s2] = send(
                        block(src, q, h), row_dev(row_of(*scaled(d2, sign2))), q, h, 6 + 2 * s + s2
                    )
        for h in range(2):
            d1, d2 = dims[h]
            got[h, 2, 0].wait_recv()
            got[h, 2, 1].wait_recv()
            src = row_of(*scaled(d1, 2))
            for s2, sign2 in enumerate((1, 3)):
                got[h, 1, 3, s2] = send(block(src, q, h), row_dev(row_of(*scaled(d2, sign2))), q, h, 10 + s2)

    def gather_second(q, got, b):
        for h in range(2):
            d1, d2 = dims[h]
            base = scaled(d1, (0, 3, 1, 2)[b])
            for s, sign in enumerate((1, 3)):
                got[h, 1, b, s].wait_recv()
                src = row_of(*added(base, scaled(d2, 4 - sign)))
                got[h, 3, b, s] = send(
                    halfblock(src, q, h, s), row_dev(row_of(*scaled(d2, sign))), q, h, 12 + 2 * b + s
                )

    pending = []
    for q in range(CHUNKS):
        if q:
            item_mask(q)
        x = x_items[:, starts[q]:starts[q + 1]]
        x_bf = x.astype(BF16)
        r = -ridge_item * x
        if q == 0:
            arrive(0)
            arrive(1)
        for t in range(4):
            if q == 0:
                settle(t)
            r = r + item_residual(x_bf, q, t)
            if q == 0 and t < 2:
                arrive(t + 2)
        p = r
        rr = jnp.sum(r * r, axis=0, keepdims=True)

        def item_step(_, state):
            x, r, p, rr = state
            g = item_product(p.astype(BF16), q) + ridge_item * p
            a = rr / jnp.sum(p * g, axis=0, keepdims=True)
            x = x + a * p
            r = r - a * g
            rn = jnp.sum(r * r, axis=0, keepdims=True)
            p = r + (rn / rr) * p
            return x, r, p, rn

        x, r, p, rr = lax.fori_loop(0, CG_STEPS - 1, item_step, (x, r, p, rr))
        g = item_product(p.astype(BF16), q) + ridge_item * p
        x = x + (rr / jnp.sum(p * g, axis=0, keepdims=True)) * p
        first = pl.multiple_of(row * own_items + starts[q], 128)
        item_out[pl.ds(first, widths[q]), :] = x.T
        pending.append(gather_own(q))

    for q in range(CHUNKS):
        gather_first(q, pending[q])
    for b in range(4):
        for q in range(CHUNKS):
            gather_second(q, pending[q], b)
    for q in range(CHUNKS):
        for h in range(2):
            for b in range(4):
                for s in range(2):
                    pending[q][h, 3, b, s].wait_recv()
    for c in started:
        c.wait_send()
    w_copy.wait()


def solution(mesh):
    grid_spec = P(("part", "row"), "col")
    user_spec = P(("part", "row"), None)
    item_spec = P(("part", "col"), None)

    def local_step(ratings, mask, user_init, item_init):
        users, items = ratings.shape
        rank = user_init.shape[1]
        own_items = items // NROW
        all_users = users * NROW
        starts = chunk_starts(own_items)
        widths = [starts[q + 1] - starts[q] for q in range(CHUNKS)]
        half_users = users // 2
        peers = len(OFFSETS)
        dma = pltpu.SemaphoreType.DMA
        hbm = pl.BlockSpec(memory_space=pltpu.HBM)
        vmem = pl.BlockSpec(memory_space=pltpu.VMEM)
        return pl.pallas_call(
            kernel,
            out_shape=(pltpu.VMEM((users, rank), F32), pltpu.VMEM((items, rank), F32)),
            in_specs=[hbm] * 4,
            out_specs=(vmem, vmem),
            scratch_shapes=[
                pltpu.VMEM((users, items), F32),
                pltpu.VMEM((users, items), jnp.int32),
                pltpu.VMEM((items, rank), F32),
                pltpu.VMEM((users, rank), F32),
                pltpu.VMEM((items, rank), BF16),
                pltpu.VMEM((rank, items), BF16),
                pltpu.VMEM((users, items), BF16),
                *[pltpu.VMEM((peers, users, w), F32) for w in widths],
                *[pltpu.VMEM((all_users, w), F32) for w in widths],
                *[pltpu.VMEM((all_users, w), BF16) for w in widths],
                pltpu.VMEM((all_users, max(widths)), BF16),
                pltpu.VMEM((2, half_users, items), BF16),
                pltpu.VMEM((CG_STEPS + 1, half_users, rank), F32),
                pltpu.VMEM((CG_STEPS + 1, half_users, rank), F32),
                pltpu.VMEM((CG_STEPS + 1, half_users, rank), F32),
                pltpu.VMEM((CG_STEPS + 1, NX - 1, half_users, rank), F32),
                pltpu.VMEM((CG_STEPS, users, rank), BF16),
                pltpu.VMEM((all_users, rank), BF16),
                pltpu.VMEM((rank, all_users), BF16),
                pltpu.VMEM((rank, own_items), F32),
                dma((2, NROW)),
                dma,
                dma((8,)),
                dma((CHUNKS, peers)),
                dma((CHUNKS, peers)),
                dma((CG_STEPS + 1,)),
                dma((CG_STEPS + 1,)),
                dma((CG_STEPS + 1, NX - 1)),
                dma((CG_STEPS + 1, NX - 1)),
                dma((CG_STEPS,)),
                dma((CG_STEPS,)),
                dma,
                dma,
                dma((peers,)),
                dma((peers,)),
                dma((NROW,)),
                dma((NROW,)),
                dma((CHUNKS, 2, 20)),
                dma((CHUNKS, 2, 20)),
            ],
            compiler_params=pltpu.CompilerParams(
                collective_id=0, has_side_effects=True, vmem_limit_bytes=48 * 2**20
            ),
            name="als_sweep",
        )(ratings, mask, pltpu.with_memory_space_constraint(user_init, pltpu.HBM), item_init)

    return jax.shard_map(
        local_step,
        mesh=mesh,
        in_specs=(grid_spec, grid_spec, user_spec, item_spec),
        out_specs=(user_spec, item_spec),
        check_vma=False,
    )
```
